512 devices in a mesh: gx: 16 (over z), gy: 16 (over x, y_hi, core), gz: 2 (over y_lo).
Axes of the slice: x: 4, y: 4 (y_hi: 2, y_lo: 2; y = y_hi * 2 + y_lo), z: 16, core: 2. Of those that a mesh axis runs over, the one named last changes fastest.
Arguments:
- displacement: float32 [3, 16, 512, 2048], P(None, 'gz', 'gx', 'gy'), may hold values from -6 to 6
- load: float32 [3, 16, 512, 2048], P(None, 'gz', 'gx', 'gy'), may hold values from -6 to 6
- density_code: int32 [16, 512, 2048], P('gz', 'gx', 'gy'), may hold values from 0 to 15
- fixed_mask: int32 [3, 16, 512, 2048], P(None, 'gz', 'gx', 'gy'), may hold values from 0 to 1, as said below
Outputs:
- improved: float32 [3, 16, 512, 2048], P(None, 'gz', 'gx', 'gy')
The draws below stay inside these ranges and needn't reach their ends.
Inputs may be any that keep to these rules, and one draw needn't show every extreme that they name: `fixed_mask`: 1 on all three components of the nodes of a few rectangular support patches in the first layer along the first dimension, and on a few scattered components elsewhere.
All inputs are finite; a program needn't handle non-finite values.
Results may differ from the reference program's by a relative error of at most 0.0001.
Values sent between devices are 32-bit elements; how exact they have to be, the bound alone decides.
No kernel may reach another device: no remote copies, remote signals or barrier semaphores. Data moves between devices by JAX's collectives and lax.ppermute only.
A program may use at most 128 MiB of HBM per device.

```python
import functools
import jax
import jax.numpy as jnp
import numpy as np

NU = 2
COARSE = 4
LEVELS = 16
NX = 512
NY = 2048
NZ = 16


def draw_fixed_mask(key, part):
    patches = 6
    wide_x = max(NX // 8, 1)
    wide_y = max(NY // 8, 1)
    first_key = jax.random.fold_in(key, 101)
    second_key = jax.random.fold_in(key, 202)
    third_key = jax.random.fold_in(key, 303)
    start_x = jax.random.randint(first_key, (patches,), 0, NX - wide_x + 1)
    start_y = jax.random.randint(second_key, (patches,), 0, NY - wide_y + 1)
    along_x = jnp.arange(NX, dtype=jnp.int32)
    along_y = jnp.arange(NY, dtype=jnp.int32)
    inside_x = (along_x[None, :] >= start_x[:, None]) & (along_x[None, :] < start_x[:, None] + wide_x)
    inside_y = (along_y[None, :] >= start_y[:, None]) & (along_y[None, :] < start_y[:, None] + wide_y)
    patch = jnp.any(inside_x[:, :, None] & inside_y[:, None, :], axis=0)
    bottom = jnp.arange(NZ, dtype=jnp.int32) == 0
    support = bottom[:, None, None] & patch[None, :, :]
    scattered = jax.random.randint(third_key, (3, NZ, NX, NY), 0, 1024) == 0
    fixed = support[None] | scattered
    return fixed.astype(jnp.int32)


def set_ends(entries, stream_key, smallest, top_value):
    shape = entries.shape
    index_at = [jax.random.randint(jax.random.fold_in(stream_key, axis), (), 0, shape[axis]) for axis in range(len(shape))]
    entries = entries.at[tuple(index_at)].set(smallest)
    longest = shape.index(max(shape))
    index_at[longest] = (index_at[longest] + 1) % shape[longest]
    return entries.at[tuple(index_at)].set(top_value)


def block_levels(own_key, shape, cuts, least, high):
    factor_of = 1.0
    for dim, blocks in cuts:
        draws = jax.random.uniform(jax.random.fold_in(jax.random.fold_in(own_key, 6), dim), (blocks,), jnp.float32, least / len(cuts), high / len(cuts))
        factor_of = factor_of * jnp.repeat(jnp.exp(draws), shape[dim] // blocks).reshape((-1,) + (1,) * (len(shape) - 1 - dim))
    return factor_of


def normal_values(stream_key, dims, deviation, bound, split=(), held_as=jnp.bfloat16):
    values = deviation * jax.random.normal(stream_key, dims, jnp.float32)
    if split:
        values = values * block_levels(stream_key, dims, split, -0.22, 0.18)
    return jnp.clip(values, -bound, bound).astype(held_as)


def setup_inputs(seed: int = 0) -> dict:
    seeds = jax.random.split(jax.random.key(seed), 5)
    displacement = normal_values(seeds[0], (3, NZ, NX, NY), 1.0, 6.0, ((1, 2), (2, 16), (3, 16)), jnp.float32)
    load = normal_values(seeds[1], (3, NZ, NX, NY), 1.0, 6.0, ((1, 2), (2, 16), (3, 16)), jnp.float32)
    density_code = set_ends(jax.random.randint(seeds[2], (NZ, NX, NY), 0, LEVELS), jax.random.fold_in(seeds[2], 1), 0, LEVELS - 1).astype(jnp.int32)
    fixed_mask = draw_fixed_mask(jax.random.fold_in(seeds[4], 71), 0)
    return {"displacement": displacement, "load": load, "density_code": density_code, "fixed_mask": fixed_mask}


EMIN = 0.001
OMEGA = 0.5

def corner(index):
    return (index >> 2 & 1, index >> 1 & 1, index & 1)

def element_matrix():
    poisson = 0.3
    lame_first = poisson / ((1 + poisson) * (1 - 2 * poisson))
    shear = 1 / (2 * (1 + poisson))
    elastic = np.zeros((6, 6))
    elastic[:3, :3] = lame_first
    for d in range(3):
        elastic[d, d] = lame_first + 2 * shear
        elastic[3 + d, 3 + d] = shear
    offset_gauss = 0.5 / np.sqrt(3.0)
    points = (0.5 - offset_gauss, 0.5 + offset_gauss)
    stiffness = np.zeros((24, 24))
    for px in points:
        for py in points:
            for pz in points:
                place = (px, py, pz)
                strain = np.zeros((6, 24))
                for a in range(8):
                    o = corner(a)
                    shapes = [place[d] if o[d] else 1 - place[d] for d in range(3)]
                    slopes = [1.0 if o[d] else -1.0 for d in range(3)]
                    gradient = [slopes[0] * shapes[1] * shapes[2], shapes[0] * slopes[1] * shapes[2], shapes[0] * shapes[1] * slopes[2]]
                    c = 3 * a
                    strain[0, c] = gradient[0]
                    strain[1, c + 1] = gradient[1]
                    strain[2, c + 2] = gradient[2]
                    strain[3, c] = gradient[1]
                    strain[3, c + 1] = gradient[0]
                    strain[4, c + 1] = gradient[2]
                    strain[4, c + 2] = gradient[1]
                    strain[5, c] = gradient[2]
                    strain[5, c + 2] = gradient[0]
                stiffness += strain.T @ elastic @ strain / 8.0
    return stiffness

def stencil(padded_u, padded_s, spacing):
    stiffness = element_matrix()
    extent = (padded_s.shape[0] - 2, padded_s.shape[1] - 2, padded_s.shape[2] - 2)

    def window(array, start):
        return array[..., start[0]:start[0] + extent[0], start[1]:start[1] + extent[1], start[2]:start[2] + extent[2]]
    forces = [None, None, None]
    diagonal = [None, None, None]
    for a in range(8):
        oa = corner(a)
        weight = window(padded_s, tuple((1 - oa[d] for d in range(3))))
        for i in range(3):
            terms = []
            for b in range(8):
                ob = corner(b)
                moved = tuple((1 - oa[d] + ob[d] for d in range(3)))
                for j in range(3):
                    coeff = float(stiffness[3 * a + i, 3 * b + j])
                    if abs(coeff) > 1e-12:
                        terms.append(coeff * window(padded_u[j], moved))
            part = weight * functools.reduce(jnp.add, terms)
            forces[i] = part if forces[i] is None else forces[i] + part
            piece = float(stiffness[3 * a + i, 3 * a + i]) * weight
            diagonal[i] = piece if diagonal[i] is None else diagonal[i] + piece
    return (spacing * jnp.stack(forces), spacing * jnp.stack(diagonal))

def global_apply(scales, spacing):
    padded_s = jnp.pad(scales, 1)

    def apply(field):
        return stencil(jnp.pad(field, ((0, 0), (1, 1), (1, 1), (1, 1))), padded_s, spacing)
    return apply

def smooth(field, rhs, free, apply, sweeps):
    for sweep in range(sweeps):
        product, diagonal = apply(field)
        field = field + OMEGA * free * (rhs - product) / diagonal
    return field

def residual(field, rhs, free, apply):
    product, diagonal = apply(field)
    return free * (rhs - product)

def coarsen(array, reducer):
    lead = array.shape[:-3]
    ex, ey, ez = array.shape[-3:]
    shaped = array.reshape(lead + (ex // 2, 2, ey // 2, 2, ez // 2, 2))
    return reducer(shaped, axis=(-5, -3, -1))

def refine(array):
    return jnp.repeat(jnp.repeat(jnp.repeat(array, 2, -3), 2, -2), 2, -1)

def reference(displacement, load, density_code, fixed_mask):
    free0 = 1.0 - fixed_mask.astype(jnp.float32)
    level = density_code.astype(jnp.float32) / (LEVELS - 1)
    scales0 = EMIN + (1.0 - EMIN) * level * level * level
    apply0 = global_apply(scales0, 1.0)
    state = smooth(free0 * displacement, load, free0, apply0, NU)
    rhs1 = coarsen(residual(state, load, free0, apply0), jnp.sum)
    scales1 = coarsen(scales0, jnp.mean)
    free1 = coarsen(free0, jnp.min)
    apply1 = global_apply(scales1, 2.0)
    corr1 = smooth(jnp.zeros_like(rhs1), rhs1, free1, apply1, NU)
    rhs2 = coarsen(residual(corr1, rhs1, free1, apply1), jnp.sum)
    scales2 = coarsen(scales1, jnp.mean)
    free2 = coarsen(free1, jnp.min)
    apply2 = global_apply(scales2, 4.0)
    corr2 = smooth(jnp.zeros_like(rhs2), rhs2, free2, apply2, COARSE)
    corr1 = smooth(corr1 + free1 * refine(corr2), rhs1, free1, apply1, NU)
    return smooth(state + free0 * refine(corr1), load, free0, apply0, NU)
```

```python
import jax
import jax.numpy as jnp
from jax import lax
from jax.experimental import pallas as pl
from jax.experimental.pallas import tpu as pltpu
from jax.sharding import PartitionSpec as P

LEVELS = 16
COARSE = 4
EMIN = 0.001
OMEGA = 0.5

POISSON = 0.3
LAME = POISSON / ((1 + POISSON) * (1 - 2 * POISSON))
SHEAR = 1 / (2 * (1 + POISSON))
KDIAG = (LAME + 4 * SHEAR) / 16 + 2 * (LAME + 3 * SHEAR) / 48 + 2 * SHEAR / 48 + (LAME + 4 * SHEAR) / 144

PLANES, ROWS, LANES = 14, 40, 256
OWN = 3
EDGE = 4
EDGE1 = 12

F32 = jnp.float32


def element(c, s):
    s16l, s16m = s * (LAME / 16), s * (SHEAR / 16)
    s16n = s * (2 * SHEAR / 16)
    s48l, s48m, s48n = s * (LAME / 48), s * (SHEAR / 48), s * ((LAME + 3 * SHEAR) / 48)
    s144 = s * ((LAME + 4 * SHEAR) / 144)

    def at(*dims):
        return tuple(1 if d in dims else 0 for d in range(3))

    g = {}
    trace = s16l * (c[0, at(0)] + c[1, at(1)] + c[2, at(2)])
    for i in range(3):
        g[i, at(i)] = s16n * c[i, at(i)] + trace
    for i, j in ((0, 1), (0, 2), (1, 2)):
        force = s16m * (c[i, at(j)] + c[j, at(i)])
        g[i, at(j)] = force
        g[j, at(i)] = force
    for j in range(3):
        i, k = [d for d in range(3) if d != j]
        first, second = c[i, at(i, j)], c[k, at(k, j)]
        g[i, at(i, j)] = s48n * first + s48l * second
        g[k, at(k, j)] = s48n * second + s48l * first
    twists = [c[i, at(*[d for d in range(3) if d != i])] for i in range(3)]
    total = twists[0] + twists[1] + twists[2]
    for i in range(3):
        g[i, at(*[d for d in range(3) if d != i])] = s48m * (twists[i] + total)
        g[i, (1, 1, 1)] = s144 * c[i, (1, 1, 1)]
    return g


def stencil(u_ref, s_ref, emit, first, count, tiles, y_ref, x_ref, hi_ref, q_ref):
    width = u_ref.shape[-1]
    parts = width // 128

    def lanes(part):
        return pl.ds(128 * part, 128)

    def spread_y(z):
        for t in tiles:
            rows = pl.ds(8 * t, 8)
            for c in range(3):
                u = u_ref[c, z, rows, :]
                after = pltpu.roll(u, width - 1, 1)
                for k, value in enumerate((u + after, after - u)):
                    for part in range(parts):
                        y_ref[2 * c + k, part, rows, :] = value[:, 128 * part: 128 * part + 128]

    def spread_x(t, part):
        out = []
        for k in range(6):
            here = y_ref[k, part, pl.ds(8 * t, 8), :]
            after = y_ref[k, part, pl.ds(8 * t + 1, 8), :]
            out += [here + after, after - here]
        return out

    spread_y(first - 1)
    for t in tiles:
        for part in range(parts):
            for i, value in enumerate(spread_x(t, part)):
                x_ref[i, part, pl.ds(8 * t, 8), :] = value

    def layer(step, carry):
        e = first - 1 + step
        spread_y(e + 1)
        for t in tiles:
            rows = pl.ds(8 * t, 8)
            sums = [[], [], []]
            for part in range(parts):
                here = lanes(part)
                c = {}
                for i, now in enumerate(spread_x(t, part)):
                    comp, yt, xt = i // 4, i // 2 % 2, i % 2
                    before = x_ref[i, part, rows, :]
                    x_ref[i, part, rows, :] = now
                    c[comp, (0, xt, yt)] = now + before
                    c[comp, (1, xt, yt)] = now - before
                g = element(c, s_ref[e, rows, here])
                for comp in range(3):
                    ends = []
                    for yt in range(2):
                        node = []
                        for xt in range(2):
                            i = 4 * comp + 2 * yt + xt
                            d = g[comp, (1, xt, yt)]
                            a = g.get((comp, (0, xt, yt)))
                            low = hi_ref[i, part, rows, :]
                            if a is None:
                                node.append(low - d)
                                hi_ref[i, part, rows, :] = d
                            else:
                                node.append(low + (a - d))
                                hi_ref[i, part, rows, :] = a + d
                        k = 2 * comp + yt
                        q_ref[k, part, pl.ds(8 * t + 1, 8), :] = node[0] + node[1]
                        ends.append(node[0] - node[1] + q_ref[k, part, rows, :])
                    sums[comp].append(ends)
            forces = []
            for comp in range(3):
                low = jnp.concatenate([a - d for a, d in sums[comp]], 1) if parts > 1 else sums[comp][0][0] - sums[comp][0][1]
                high = jnp.concatenate([a + d for a, d in sums[comp]], 1) if parts > 1 else sums[comp][0][0] + sums[comp][0][1]
                forces.append(low + pltpu.roll(high, 1, 1))
            emit(e, t, forces)
        return carry

    lax.fori_loop(0, count + 1, layer, 0)


def box_inverse(total, factor):
    positive = total > 0
    return jnp.where(positive, OMEGA / (factor * jnp.where(positive, total, 1.0)), 0.0)


def lane_index(shape):
    return lax.broadcasted_iota(jnp.int32, shape, len(shape) - 1)


def call(body, outs, args, scratch=(), in_specs=None, out_specs=None):
    whole = pl.BlockSpec(memory_space=pltpu.VMEM)
    specs = [pl.BlockSpec(memory_space=pltpu.SMEM)] + [whole] * (len(args) - 1)
    return pl.pallas_call(
        body,
        out_shape=tuple(
            jax.ShapeDtypeStruct(shape, F32) if body is coarse else pltpu.VMEM(shape, F32) for shape in outs
        ),
        in_specs=in_specs or specs,
        out_specs=out_specs or tuple(whole for _ in outs),
        scratch_shapes=list(scratch),
        compiler_params=pltpu.CompilerParams(vmem_limit_bytes=24 * 1024 * 1024),
    )(args[0], *(value if body is prepare else pltpu.with_memory_space_constraint(value, pltpu.VMEM) for value in args[1:]))


def prepare(gz_ref, disp_ref, load_ref, code_ref, fixed_ref, base_ref, send_ref):
    gz = gz_ref[0]
    for z in range(8):
        level = code_ref[z].astype(F32) / (LEVELS - 1)
        base_ref[9, z] = EMIN + (1.0 - EMIN) * level * level * level
        for c in range(3):
            free = 1.0 - fixed_ref[c, z].astype(F32)
            base_ref[c, z] = free * disp_ref[c, z]
            base_ref[3 + c, z] = load_ref[c, z]
            base_ref[6 + c, z] = free
    three, two = 5 * (1 - gz), 6 * (1 - gz)
    for c in range(3):
        for j in range(3):
            send_ref[3 * c + j] = base_ref[c, three + j]
        for j in range(2):
            send_ref[9 + 2 * c + j] = base_ref[3 + c, two + j]
            send_ref[15 + 2 * c + j] = base_ref[6 + c, two + j]
    for j in range(3):
        send_ref[21 + j] = base_ref[9, three + j]


def edge_rows(gz_ref, base_ref, zrecv_ref, right_ref, left_ref):
    for k in range(104):
        if k < 80:
            f, z = divmod(k, 8)
            right_ref[pl.ds(4 * k, 4)] = base_ref[f, z, pl.ds(28, 4)]
            left_ref[pl.ds(4 * k, 4)] = base_ref[f, z, pl.ds(0, 4)]
        else:
            right_ref[pl.ds(4 * k, 4)] = zrecv_ref[k - 80, pl.ds(28, 4)]
            left_ref[pl.ds(4 * k, 4)] = zrecv_ref[k - 80, pl.ds(0, 4)]


def fine_places(gz):
    places = [(f, OWN + z) for f in range(10) for z in range(8)]
    three, two = 11 * (1 - gz), 11 - 10 * gz
    places += [(c, three + j) for c in range(3) for j in range(3)]
    places += [(3 + c, two + j) for c in range(3) for j in range(2)]
    places += [(6 + c, two + j) for c in range(3) for j in range(2)]
    places += [(9, three + j) for j in range(3)]
    return places


def edge_lanes(gz_ref, base_ref, zrecv_ref, low_ref, high_ref, ext_ref, send_ref):
    gz = gz_ref[0]
    blank = jnp.zeros((ROWS, 128), F32)
    for f in range(10):
        for z in list(range(OWN)) + list(range(OWN + 8, PLANES)):
            ext_ref[f, z] = blank
    lane = lane_index((ROWS, 128))
    packed = None
    for k, (f, z) in enumerate(fine_places(gz)):
        ext_ref[f, z, pl.ds(0, 4)] = low_ref[pl.ds(4 * k, 4)]
        ext_ref[f, z, pl.ds(4, 32)] = base_ref[k // 8, k % 8] if k < 80 else zrecv_ref[k - 80]
        ext_ref[f, z, pl.ds(36, 4)] = high_ref[pl.ds(4 * k, 4)]
        group = k % 16
        value = ext_ref[f, z]
        if group == 0:
            packed = value
        else:
            packed = jnp.where((lane >= 8 * group - 4) & (lane < 8 * group + 4), pltpu.roll(value, 8 * group, 1), packed)
        if group == 15 or k == 103:
            send_ref[k // 16] = packed


def fine_down(gz_ref, ext_ref, low_ref, high_ref,
              main_ref, send_ref, plane_ref,
              y_ref, x_ref, hi_ref, q_ref, r_ref, pair_ref, rows_ref):
    gz = gz_ref[0]
    blank = jnp.zeros((ROWS, 128), F32)
    for f in range(10):
        for z in range(PLANES):
            main_ref[f, z, :, pl.ds(0, 128)] = ext_ref[f, z]
        for z in list(range(OWN)) + list(range(OWN + 8, PLANES)):
            main_ref[f, z, :, pl.ds(128, 128)] = blank
    lane = lane_index((ROWS, 128))
    merged = None
    for k, (f, z) in enumerate(fine_places(gz)):
        group = k % 16
        if group == 0:
            merged = jnp.where(lane % 8 < 4, high_ref[k // 16], low_ref[k // 16])
        value = merged if group == 0 else pltpu.roll(merged, 128 - 8 * group, 1)
        main_ref[f, z, :, pl.ds(128, 128)] = jnp.where((lane < EDGE) | (lane >= 128 - EDGE), value, 0.0)
    for ref in (hi_ref, q_ref, y_ref):
        for k in range(ref.shape[0]):
            ref[k] = jnp.zeros(ref.shape[1:], F32)

    for c in range(3):
        for z1 in range(4):
            z = OWN + 2 * z1
            pair_ref[0] = jnp.minimum(
                main_ref[6 + c, z, :, pl.ds(0, 128)], main_ref[6 + c, z + 1, :, pl.ds(0, 128)]
            )
            least = jnp.minimum(pair_ref[0, pl.ds(4, 16, 2), :], pair_ref[0, pl.ds(5, 16, 2), :])
            rows_ref[pl.ds(32 * (4 + c) + 16 * (z1 // 2), 16), pl.ds(128 * (z1 % 2), 128)] = least

    def weigh(z, carry):
        for t in range(5):
            rows = pl.ds(8 * t, 8)
            s = main_ref[9, z, rows, :] + main_ref[9, z - 1, rows, :]
            for part in range(2):
                q_ref[0, part, pl.ds(8 * t + 1, 8), :] = s[:, 128 * part: 128 * part + 128]
            s = s + jnp.concatenate([q_ref[0, part, rows, :] for part in range(2)], 1)
            inverse = box_inverse(s + pltpu.roll(s, 1, 1), KDIAG)
            for c in range(3):
                main_ref[6 + c, z, rows, :] = main_ref[6 + c, z, rows, :] * inverse
        return carry

    lax.fori_loop(1, PLANES, weigh, 0)

    def sweep(z, t, forces):
        rows = pl.ds(8 * t, 8)
        for c in range(3):
            u = main_ref[c, z, rows, :]
            main_ref[c, z, rows, :] = u + main_ref[6 + c, z, rows, :] * (main_ref[3 + c, z, rows, :] - forces[c])

    u_ref, s_ref = main_ref, main_ref.at[9]
    tiles = range(5)

    def one(k, carry):
        stencil(u_ref, s_ref, sweep, 3 - 2 * gz + k * gz, 10 - k, tiles, y_ref, x_ref, hi_ref, q_ref)
        return carry

    lax.fori_loop(0, 2, one, 0)

    def remain(z, t, forces):
        rows = pl.ds(8 * t, 8)
        here = pl.ds(0, 128)
        for c in range(3):
            rest = main_ref[3 + c, z, rows, here] - forces[c][:, :128]
            r_ref[c, z - OWN + 1, rows, :] = jnp.where(main_ref[6 + c, z, rows, here] > 0, rest, 0.0)

    stencil(u_ref, s_ref, remain, OWN, 8, tiles, y_ref, x_ref, hi_ref, q_ref)

    for c in range(3):
        for z1 in range(4):
            pair_ref[0] = r_ref[c, 1 + 2 * z1] + r_ref[c, 2 + 2 * z1]
            total = pair_ref[0, pl.ds(4, 16, 2), :] + pair_ref[0, pl.ds(5, 16, 2), :]
            rows_ref[pl.ds(32 * c + 16 * (z1 // 2), 16), pl.ds(128 * (z1 % 2), 128)] = total
    for z1 in range(4):
        z = OWN + 2 * z1
        pair_ref[0] = main_ref[9, z, :, pl.ds(0, 128)] + main_ref[9, z + 1, :, pl.ds(0, 128)]
        total = pair_ref[0, pl.ds(4, 16, 2), :] + pair_ref[0, pl.ds(5, 16, 2), :]
        rows_ref[pl.ds(32 * 3 + 16 * (z1 // 2), 16), pl.ds(128 * (z1 % 2), 128)] = total
        box = []
        for k in range(2):
            here = pl.ds(128 * k, 128)
            pair_ref[k] = (main_ref[9, z - 2, :, here] + main_ref[9, z - 1, :, here]) + (
                main_ref[9, z, :, here] + main_ref[9, z + 1, :, here]
            )
            box.append(
                (pair_ref[k, pl.ds(2, 16, 2), :] + pair_ref[k, pl.ds(3, 16, 2), :])
                + (pair_ref[k, pl.ds(4, 16, 2), :] + pair_ref[k, pl.ds(5, 16, 2), :])
            )
        lane16 = lane_index((16, 128))
        back = jnp.where(lane16 < 2, pltpu.roll(box[1], 2, 1), pltpu.roll(box[0], 2, 1))
        rows_ref[pl.ds(32 * 7 + 16 * (z1 // 2), 16), pl.ds(128 * (z1 % 2), 128)] = box[0] + back

    source = lax.broadcasted_iota(jnp.int32, (256, 128), 0)
    target = lax.broadcasted_iota(jnp.int32, (256, 128), 1)
    join = jnp.where(source // 2 == target, 1.0, 0.0).astype(F32)
    level1 = jnp.dot(rows_ref[...], join, precision=lax.Precision.HIGHEST, preferred_element_type=F32)

    def part(k):
        return level1[32 * k: 32 * k + 32]

    inverse = box_inverse(part(7), 2.0 * KDIAG / 8)
    results = [part(0), part(1), part(2), part(3) * (2.0 / 8)]
    results += [jnp.where(part(4 + c) > 1.5, inverse, 0.0) for c in range(3)]
    for k in range(7):
        for pair in range(2):
            send_ref[k, pair] = results[k][16 * pair: 16 * pair + 16]
    away = OWN + 6 - 5 * gz
    for c in range(3):
        plane_ref[c] = main_ref[c, away]


def edge_rows1(gz_ref, own_ref, other_ref, full_ref, right_ref, left_ref):
    gz = gz_ref[0]
    for f in range(7):
        full_ref[f, pl.ds(2 * gz, 2)] = own_ref[f]
        full_ref[f, pl.ds(2 - 2 * gz, 2)] = other_ref[f]
    for f in range(7):
        for pair in range(4):
            k = 4 * f + pair
            right_ref[pl.ds(12 * k, 12)] = full_ref[f, pair, pl.ds(4, 12)]
            left_ref[pl.ds(12 * k, 12)] = full_ref[f, pair, pl.ds(0, 12)]


def edge_lanes1(gz_ref, full_ref, low_ref, high_ref, ext_ref, right_ref, left_ref):
    lane = lane_index((ROWS, 128))
    for f in range(7):
        right = left = None
        for pair in range(4):
            k = 4 * f + pair
            ext_ref[f, pair, pl.ds(0, 12)] = low_ref[pl.ds(12 * k, 12)]
            ext_ref[f, pair, pl.ds(12, 16)] = full_ref[f, pair]
            ext_ref[f, pair, pl.ds(28, 12)] = high_ref[pl.ds(12 * k, 12)]
            value = ext_ref[f, pair]
            moved = pltpu.roll(value, 16 * pair, 1) if pair else value
            place = (lane + (128 - 16 * pair)) % 64
            right = moved if right is None else jnp.where(place >= 52, moved, right)
            left = moved if left is None else jnp.where(place < 12, moved, left)
        right_ref[f] = right
        left_ref[f] = left


def coarse(gz_ref, ext_ref, low_ref, high_ref, main_ref, other_ref, out_ref,
           v1_ref, v2_ref, state_ref, y_ref, x_ref, hi_ref, q_ref, r_ref, rows_ref, pair_ref,
           fy_ref, fx_ref, fhi_ref, fq_ref):
    gz = gz_ref[0]
    lane = lane_index((ROWS, 128))
    slots = (3, 4, 5, 6, 7, 8, 9)
    for ref in (y_ref, x_ref, hi_ref, q_ref, fy_ref, fhi_ref, fq_ref):
        for k in range(ref.shape[0]):
            ref[k] = jnp.zeros(ref.shape[1:], F32)
    for f in range(10):
        for z in (0, 9):
            v1_ref[f, z] = jnp.zeros((ROWS, 128), F32)
        for z in range(6):
            v2_ref[f, z] = jnp.zeros((24, 128), F32)
    for f in range(7):
        low, high = low_ref[f], high_ref[f]
        for pair in range(4):
            value = ext_ref[f, pair]
            for half in range(2):
                own = value if half == 0 else pltpu.roll(value, 64, 1)
                turn = (64 - 16 * pair - 64 * half) % 128
                below = pltpu.roll(low, turn, 1) if turn else low
                above = pltpu.roll(high, turn, 1) if turn else high
                whole = jnp.where(
                    lane < 64, own, jnp.where(lane < 64 + EDGE1, above, jnp.where(lane >= 128 - EDGE1, below, 0.0))
                )
                v1_ref[slots[f], 1 + 2 * pair + half] = whole
    for c in range(3):
        for z in range(10):
            v1_ref[c, z] = v1_ref[7 + c, z] * v1_ref[3 + c, z]

    def smooth(v_ref):
        def sweep(z, t, forces):
            rows = pl.ds(8 * t, 8)
            for c in range(3):
                u = v_ref[c, z, rows, :]
                v_ref[c, z, rows, :] = u + v_ref[7 + c, z, rows, :] * (v_ref[3 + c, z, rows, :] - forces[c])
        return sweep

    s1_ref = v1_ref.at[6]
    stencil(v1_ref, s1_ref, smooth(v1_ref), 1, 8, range(5), y_ref, x_ref, hi_ref, q_ref)

    def remain(z, t, forces):
        rows = pl.ds(8 * t, 8)
        for c in range(3):
            rest = v1_ref[3 + c, z, rows, :] - forces[c]
            r_ref[c, z, rows, :] = jnp.where(v1_ref[7 + c, z, rows, :] > 0, rest, 0.0)

    stencil(v1_ref, s1_ref, remain, 1, 8, range(5), y_ref, x_ref, hi_ref, q_ref)

    for z2 in range(4):
        z = 1 + 2 * z2
        for c in range(3):
            r_ref[c, z] = r_ref[c, z] + r_ref[c, z + 1]
            rows_ref[pl.ds(24 * (4 * c + z2), 20)] = r_ref[c, z, pl.ds(0, 20, 2), :] + r_ref[c, z, pl.ds(1, 20, 2), :]
            r_ref[c, 9] = jnp.where((v1_ref[7 + c, z] > 0) & (v1_ref[7 + c, z + 1] > 0), 1.0, 0.0)
            rows_ref[pl.ds(24 * (16 + 4 * c + z2), 20)] = jnp.minimum(
                r_ref[c, 9, pl.ds(0, 20, 2), :], r_ref[c, 9, pl.ds(1, 20, 2), :]
            )
        r_ref[0, 9] = v1_ref[6, z] + v1_ref[6, z + 1]
        rows_ref[pl.ds(24 * (12 + z2), 20)] = r_ref[0, 9, pl.ds(0, 20, 2), :] + r_ref[0, 9, pl.ds(1, 20, 2), :]
    for k in range(28):
        rows_ref[pl.ds(24 * k + 20, 4)] = jnp.zeros((4, 128), F32)
    source = lax.broadcasted_iota(jnp.int32, (128, 128), 0)
    target = lax.broadcasted_iota(jnp.int32, (128, 128), 1)
    used = (target < 40) | (target >= 120)
    fold = (source // 2 + jnp.where(target < 64, 0, 64) == target) & used
    join = jnp.where(fold, 1.0, 0.0).astype(F32)
    level2 = jnp.dot(rows_ref[...], join, precision=lax.Precision.HIGHEST, preferred_element_type=F32)

    def part(k, z2):
        return level2[24 * (4 * k + z2): 24 * (4 * k + z2) + 24]

    for z2 in range(4):
        for c in range(3):
            v2_ref[3 + c, 1 + z2] = part(c, z2)
            v2_ref[7 + c, 1 + z2] = jnp.where(part(4 + c, z2) > 1.5, 1.0, 0.0)
        v2_ref[6, 1 + z2] = part(3, z2) * (4.0 / 2.0 / 8.0)
    for z in range(1, 5):
        for t in range(3):
            rows = pl.ds(8 * t, 8)
            s = v2_ref[6, z, rows, :] + v2_ref[6, z - 1, rows, :]
            q_ref[0, 0, pl.ds(8 * t + 1, 8), :] = s
            s = s + q_ref[0, 0, rows, :]
            inverse = box_inverse(s + pltpu.roll(s, 1, 1), KDIAG)
            for c in range(3):
                weight = v2_ref[7 + c, z, rows, :] * inverse
                v2_ref[7 + c, z, rows, :] = weight
                v2_ref[c, z, rows, :] = weight * v2_ref[3 + c, z, rows, :]

    def again(k, carry):
        stencil(v2_ref, v2_ref.at[6], smooth(v2_ref), 1, 4, range(3), y_ref, x_ref, hi_ref, q_ref)
        return carry

    lax.fori_loop(0, COARSE - 1, again, 0)

    part_of = jnp.where(
        (source == jnp.where(target < 96, target // 2, target // 2 + 64)), 1.0, 0.0
    ).astype(F32)
    for c in range(3):
        for z2 in range(4):
            rows_ref[pl.ds(24 * (4 * c + z2), 24)] = v2_ref[c, 1 + z2]
    spread = jnp.dot(rows_ref[pl.ds(0, 288)], part_of, precision=lax.Precision.HIGHEST, preferred_element_type=F32)
    for c in range(3):
        for z2 in range(4):
            k = 24 * (4 * c + z2)
            value = spread[k: k + 24][:20]
            r_ref[c, 9, pl.ds(0, 20, 2), :] = value
            r_ref[c, 9, pl.ds(1, 20, 2), :] = value
            for z in (1 + 2 * z2, 2 + 2 * z2):
                v1_ref[c, z] = v1_ref[c, z] + jnp.where(v1_ref[7 + c, z] > 0, r_ref[c, 9], 0.0)

    def second(k, carry):
        stencil(v1_ref, s1_ref, smooth(v1_ref), 1 + 2 * gz + k * gz, 6 - k, range(1, 4), y_ref, x_ref, hi_ref, q_ref)
        return carry

    lax.fori_loop(0, 2, second, 0)

    start = 4 * gz
    for c in range(3):
        for j in range(6):
            rows_ref[pl.ds(24 * (6 * c + j), 24)] = v1_ref[c, start + j, pl.ds(8, 24), :]
    target2 = lax.broadcasted_iota(jnp.int32, (128, 256), 1)
    source2 = lax.broadcasted_iota(jnp.int32, (128, 256), 0)
    copies = jnp.where(source2 == target2 // 2, 1.0, 0.0).astype(F32)
    fine = jnp.dot(rows_ref[pl.ds(0, 432)], copies, precision=lax.Precision.HIGHEST, preferred_element_type=F32)
    for c in range(3):
        for z in range(PLANES):
            state_ref[c, z] = main_ref[c, z]
        state_ref[c, 12 - 11 * gz] = other_ref[c]
        for j in range(6):
            k = 24 * (6 * c + j)
            value = fine[k: k + 24][2:22]
            for k in range(2):
                here = pl.ds(128 * k, 128)
                pair_ref[k, pl.ds(0, 20, 2), :] = value[:, 128 * k: 128 * k + 128]
                pair_ref[k, pl.ds(1, 20, 2), :] = value[:, 128 * k: 128 * k + 128]
                for half in range(2):
                    z = 1 + 2 * j + half
                    state_ref[c, z, :, here] = state_ref[c, z, :, here] + jnp.where(
                        main_ref[6 + c, z, :, here] > 0, pair_ref[k], 0.0
                    )

    def sweep(z, t, forces):
        rows = pl.ds(8 * t, 8)
        for c in range(3):
            u = state_ref[c, z, rows, :]
            state_ref[c, z, rows, :] = u + main_ref[6 + c, z, rows, :] * (main_ref[3 + c, z, rows, :] - forces[c])

    def last(k, carry):
        stencil(state_ref, main_ref.at[9], sweep, 3 - gz + k * gz, 9 - k, range(5), fy_ref, fx_ref, fhi_ref, fq_ref)
        return carry

    lax.fori_loop(0, 2, last, 0)
    for c in range(3):
        for z in range(8):
            out_ref[c, z] = state_ref[c, OWN + z, pl.ds(4, 32), pl.ds(0, 128)]


def up(value, axis):
    return lax.ppermute(value, axis, [(i, i + 1) for i in range(lax.axis_size(axis) - 1)])


def down(value, axis):
    return lax.ppermute(value, axis, [(i + 1, i) for i in range(lax.axis_size(axis) - 1)])


def swap(value):
    return lax.ppermute(value, "gz", [(0, 1), (1, 0)])


def scratch_of(rows, width):
    return [
        pltpu.VMEM((6, width // 128, rows + 8, 128), F32),
        pltpu.VMEM((12, width // 128, rows, 128), F32),
        pltpu.VMEM((12, width // 128, rows, 128), F32),
        pltpu.VMEM((6, width // 128, rows + 8, 128), F32),
    ]


def on_device(displacement, load, density_code, fixed_mask):
    gz = lax.axis_index("gz").astype(jnp.int32).reshape(1)
    base, zsend = call(
        prepare, [(10, 8, 32, 128), (24, 32, 128)], [gz, displacement, load, density_code, fixed_mask]
    )
    zrecv = swap(zsend)
    right, left = call(edge_rows, [(416, 128)] * 2, [gz, base, zrecv])
    low, high = up(right, "gx"), down(left, "gx")
    ext, ysend = call(
        edge_lanes, [(10, PLANES, ROWS, 128), (7, ROWS, 128)], [gz, base, zrecv, low, high]
    )
    low, high = up(ysend, "gy"), down(ysend, "gy")
    main, send1, plane = call(
        fine_down,
        [(10, PLANES, ROWS, LANES), (7, 2, 16, 128), (3, ROWS, LANES)],
        [gz, ext, low, high],
        scratch_of(ROWS, LANES)
        + [pltpu.VMEM((3, 9, ROWS, 128), F32), pltpu.VMEM((2, ROWS, 128), F32), pltpu.VMEM((256, 256), F32)],
    )
    other1 = swap(send1)
    other_plane = swap(plane)
    full, right, left = call(edge_rows1, [(7, 4, 16, 128), (336, 128), (336, 128)], [gz, send1, other1])
    low, high = up(right, "gx"), down(left, "gx")
    ext1, right, left = call(
        edge_lanes1, [(7, 4, ROWS, 128), (7, ROWS, 128), (7, ROWS, 128)], [gz, full, low, high]
    )
    low, high = up(right, "gy"), down(left, "gy")
    (out,) = call(
        coarse,
        [(3, 8, 32, 128)],
        [gz, ext1, low, high, main, other_plane],
        [
            pltpu.VMEM((10, 10, ROWS, 128), F32),
            pltpu.VMEM((10, 6, 24, 128), F32),
            pltpu.VMEM((3, PLANES, ROWS, LANES), F32),
        ]
        + scratch_of(ROWS, 128)
        + [pltpu.VMEM((3, 10, ROWS, 128), F32), pltpu.VMEM((672, 128), F32), pltpu.VMEM((2, ROWS, 128), F32)]
        + scratch_of(ROWS, LANES),
    )
    return out


def solution(mesh):
    return jax.shard_map(
        on_device,
        mesh=mesh,
        in_specs=(
            P(None, "gz", "gx", "gy"),
            P(None, "gz", "gx", "gy"),
            P("gz", "gx", "gy"),
            P(None, "gz", "gx", "gy"),
        ),
        out_specs=P(None, "gz", "gx", "gy"),
        check_vma=False,
    )
```

```python
import jax
import jax.numpy as jnp
from jax import lax
from jax.experimental import pallas as pl
from jax.experimental.pallas import tpu as pltpu
from jax.sharding import PartitionSpec as P

LEVELS = 16
COARSE = 4
EMIN = 0.001
OMEGA = 0.5

POISSON = 0.3
LAME = POISSON / ((1 + POISSON) * (1 - 2 * POISSON))
SHEAR = 1 / (2 * (1 + POISSON))
KDIAG = (LAME + 4 * SHEAR) / 16 + 2 * (LAME + 3 * SHEAR) / 48 + 2 * SHEAR / 48 + (LAME + 4 * SHEAR) / 144

PLANES, ROWS, LANES = 14, 40, 256
OWN = 3
EDGE = 4
EDGE1 = 12

F32 = jnp.float32


def element(c, s):
    s16l, s16m = s * (LAME / 16), s * (SHEAR / 16)
    s16n = s * (2 * SHEAR / 16)
    s48l, s48m, s48n = s * (LAME / 48), s * (SHEAR / 48), s * ((LAME + 3 * SHEAR) / 48)
    s144 = s * ((LAME + 4 * SHEAR) / 144)

    def at(*dims):
        return tuple(1 if d in dims else 0 for d in range(3))

    g = {}
    trace = s16l * (c[0, at(0)] + c[1, at(1)] + c[2, at(2)])
    for i in range(3):
        g[i, at(i)] = s16n * c[i, at(i)] + trace
    for i, j in ((0, 1), (0, 2), (1, 2)):
        force = s16m * (c[i, at(j)] + c[j, at(i)])
        g[i, at(j)] = force
        g[j, at(i)] = force
    for j in range(3):
        i, k = [d for d in range(3) if d != j]
        first, second = c[i, at(i, j)], c[k, at(k, j)]
        g[i, at(i, j)] = s48n * first + s48l * second
        g[k, at(k, j)] = s48n * second + s48l * first
    twists = [c[i, at(*[d for d in range(3) if d != i])] for i in range(3)]
    total = twists[0] + twists[1] + twists[2]
    for i in range(3):
        g[i, at(*[d for d in range(3) if d != i])] = s48m * (twists[i] + total)
        g[i, (1, 1, 1)] = s144 * c[i, (1, 1, 1)]
    return g


def stencil(u_ref, s_ref, emit, first, count, tiles, y_ref, x_ref, hi_ref, q_ref, r_ref):
    width = u_ref.shape[-1]
    parts = width // 128

    def split(value):
        return [value[:, 128 * part: 128 * part + 128] for part in range(parts)]

    def join(values):
        return jnp.concatenate(values, 1) if parts > 1 else values[0]

    for j in range(count + 2):
        for t in tiles:
            rows = pl.ds(8 * t, 8)
            for c in range(3):
                u = u_ref[c, first - 1 + j, rows, :]
                after = pltpu.roll(u, width - 1, 1)
                for k, value in enumerate((u + after, after - u)):
                    for part, piece in enumerate(split(value)):
                        y_ref[j, 2 * c + k, part, rows, :] = piece

    def spread_x(j, t, part):
        out = []
        for k in range(6):
            here = y_ref[j, k, part, pl.ds(8 * t, 8), :]
            after = y_ref[j, k, part, pl.ds(8 * t + 1, 8), :]
            out += [here + after, after - here]
        return out

    for t in tiles:
        for part in range(parts):
            for i, value in enumerate(spread_x(0, t, part)):
                x_ref[i, part, pl.ds(8 * t, 8), :] = value

    def layer(step, carry):
        e = first - 1 + step
        for t in tiles:
            rows = pl.ds(8 * t, 8)
            for part in range(parts):
                c = {}
                for i, now in enumerate(spread_x(step + 1, t, part)):
                    comp, yt, xt = i // 4, i // 2 % 2, i % 2
                    before = x_ref[i, part, rows, :]
                    x_ref[i, part, rows, :] = now
                    c[comp, (0, xt, yt)] = now + before
                    c[comp, (1, xt, yt)] = now - before
                g = element(c, s_ref[e, rows, pl.ds(128 * part, 128)])
                for comp in range(3):
                    ends = []
                    for yt in range(2):
                        node = []
                        for xt in range(2):
                            i = 4 * comp + 2 * yt + xt
                            d = g[comp, (1, xt, yt)]
                            a = g.get((comp, (0, xt, yt)))
                            low = hi_ref[i, part, rows, :]
                            if a is None:
                                node.append(low - d)
                                hi_ref[i, part, rows, :] = d
                            else:
                                node.append(low + (a - d))
                                hi_ref[i, part, rows, :] = a + d
                        k = 2 * comp + yt
                        q_ref[k, part, pl.ds(8 * t + 1, 8), :] = node[0] + node[1]
                        ends.append(node[0] - node[1] + q_ref[k, part, rows, :])
                    r_ref[step, 2 * comp, part, rows, :] = ends[0] - ends[1]
                    r_ref[step, 2 * comp + 1, part, rows, :] = ends[0] + ends[1]
        return carry

    lax.fori_loop(0, count + 1, layer, 0)

    for j in range(count):
        for t in tiles:
            rows = pl.ds(8 * t, 8)
            forces = []
            for comp in range(3):
                low = join([r_ref[j + 1, 2 * comp, part, rows, :] for part in range(parts)])
                high = join([r_ref[j + 1, 2 * comp + 1, part, rows, :] for part in range(parts)])
                forces.append(low + pltpu.roll(high, 1, 1))
            emit(first + j, t, forces)


def smoother(u_ref, rhs_ref, weight_ref):
    def sweep(z, t, forces):
        rows = pl.ds(8 * t, 8)
        for c in range(3):
            u = u_ref[c, z, rows, :]
            u_ref[c, z, rows, :] = u + weight_ref[c, z, rows, :] * (rhs_ref[c, z, rows, :] - forces[c])

    return sweep


def box_inverse(total, factor):
    positive = total > 0
    return jnp.where(positive, OMEGA / (factor * jnp.where(positive, total, 1.0)), 0.0)


def clear(*refs):
    for ref in refs:
        for k in range(ref.shape[0]):
            ref[k] = jnp.zeros(ref.shape[1:], F32)


def clear_work(y_ref, x_ref, hi_ref, q_ref, r_ref):
    planes, six, parts, rows, _ = y_ref.shape
    for j in range(planes):
        y_ref[j, :, :, pl.ds(rows - 8, 8), :] = jnp.zeros((six, parts, 8, 128), F32)
    clear(hi_ref, q_ref)


def lane_index(shape):
    return lax.broadcasted_iota(jnp.int32, shape, len(shape) - 1)


def call(body, outs, args, scratch=(), inputs="vmem", output="vmem"):
    whole = pl.BlockSpec(memory_space=pltpu.VMEM)
    rest = pl.BlockSpec(memory_space=pltpu.HBM) if inputs == "any" else whole
    values = args[1:]
    if inputs == "vmem":
        values = [pltpu.with_memory_space_constraint(value, pltpu.VMEM) for value in values]
    shape = pltpu.VMEM if output == "vmem" else jax.ShapeDtypeStruct
    return pl.pallas_call(
        body,
        out_shape=tuple(shape(out, F32) for out in outs),
        in_specs=[pl.BlockSpec(memory_space=pltpu.SMEM)] + [rest] * len(values),
        out_specs=tuple(whole for _ in outs),
        scratch_shapes=list(scratch),
        compiler_params=pltpu.CompilerParams(vmem_limit_bytes=24 * 1024 * 1024),
    )(args[0], *values)


def scale_of(code):
    level = code.astype(F32) / (LEVELS - 1)
    return EMIN + (1.0 - EMIN) * level * level * level


def boundary(gz_ref, disp_ref, load_ref, code_ref, fixed_ref, send_ref, disp, load, code, fixed, sems):
    gz = gz_ref[0]
    three, two = 5 * (1 - gz), 6 * (1 - gz)
    copies = [
        pltpu.make_async_copy(code_ref.at[pl.ds(three, 3)], code, sems.at[0]),
        pltpu.make_async_copy(fixed_ref.at[:, pl.ds(three, 3)], fixed, sems.at[1]),
        pltpu.make_async_copy(disp_ref.at[:, pl.ds(three, 3)], disp, sems.at[2]),
        pltpu.make_async_copy(load_ref.at[:, pl.ds(two, 2)], load, sems.at[3]),
    ]
    for copy in copies:
        copy.start()
    for copy in copies:
        copy.wait()
    for j in range(3):
        send_ref[21 + j] = scale_of(code[j])
        for c in range(3):
            send_ref[3 * c + j] = (1.0 - fixed[c, j].astype(F32)) * disp[c, j]
    for c in range(3):
        for j in range(2):
            send_ref[9 + 2 * c + j] = load[c, j]
            send_ref[15 + 2 * c + j] = 1.0 - fixed[c, j + 1 - gz].astype(F32)


def prepare(gz_ref, disp_ref, load_ref, code_ref, fixed_ref, base_ref, right_ref, left_ref):
    for z in range(8):
        base_ref[9, z] = scale_of(code_ref[z])
        for c in range(3):
            free = 1.0 - fixed_ref[c, z].astype(F32)
            base_ref[c, z] = free * disp_ref[c, z]
            base_ref[3 + c, z] = load_ref[c, z]
            base_ref[6 + c, z] = free
    for k in range(80):
        right_ref[pl.ds(4 * k, 4)] = base_ref[k // 8, k % 8, pl.ds(28, 4)]
        left_ref[pl.ds(4 * k, 4)] = base_ref[k // 8, k % 8, pl.ds(0, 4)]


def boundary_rows(gz_ref, low_ref, high_ref, send_ref):
    lower = gz_ref[0] == 0

    def send(k, f, below, above):
        for i, ref in enumerate((low_ref, high_ref)):
            first, second = 4 * (8 * f + below), 4 * (8 * f + above)
            send_ref[pl.ds(8 * k + 4 * i, 4)] = jnp.where(lower, ref[pl.ds(first, 4)], ref[pl.ds(second, 4)])

    for j in range(3):
        send(21 + j, 9, 5 + j, j)
        for c in range(3):
            send(3 * c + j, c, 5 + j, j)
    for c in range(3):
        for j in range(2):
            send(9 + 2 * c + j, 3 + c, 6 + j, j)
            send(15 + 2 * c + j, 6 + c, 6 + j, j)


def fine_places(gz):
    places = [(f, OWN + z) for f in range(10) for z in range(8)]
    three, two = 11 * (1 - gz), 11 - 10 * gz
    places += [(c, three + j) for c in range(3) for j in range(3)]
    places += [(3 + c, two + j) for c in range(3) for j in range(2)]
    places += [(6 + c, two + j) for c in range(3) for j in range(2)]
    places += [(9, three + j) for j in range(3)]
    return places


def edge_lanes(gz_ref, base_ref, zrecv_ref, low_ref, high_ref, beside_ref, ext_ref, send_ref):
    gz = gz_ref[0]
    blank = jnp.zeros((ROWS, 128), F32)
    for f in range(10):
        for z in list(range(OWN)) + list(range(OWN + 8, PLANES)):
            ext_ref[f, z] = blank
    lane = lane_index((ROWS, 128))
    packed = None
    for k, (f, z) in enumerate(fine_places(gz)):
        beside = 8 * (k - 80)
        ext_ref[f, z, pl.ds(0, 4)] = low_ref[pl.ds(4 * k, 4)] if k < 80 else beside_ref[pl.ds(beside, 4)]
        ext_ref[f, z, pl.ds(4, 32)] = base_ref[k // 8, k % 8] if k < 80 else zrecv_ref[k - 80]
        ext_ref[f, z, pl.ds(36, 4)] = high_ref[pl.ds(4 * k, 4)] if k < 80 else beside_ref[pl.ds(beside + 4, 4)]
        group = k % 16
        value = ext_ref[f, z]
        if group == 0:
            packed = value
        else:
            packed = jnp.where((lane >= 8 * group - 4) & (lane < 8 * group + 4), pltpu.roll(value, 8 * group, 1), packed)
        if group == 15 or k == 103:
            send_ref[k // 16] = packed


def fine_down(gz_ref, ext_ref, low_ref, high_ref,
              u_ref, load_ref, weight_ref, s_ref, send_ref, plane_ref,
              y_ref, x_ref, hi_ref, q_ref, r_ref, rest_ref, pair_ref, rows_ref):
    gz = gz_ref[0]
    blank = jnp.zeros((ROWS, 128), F32)
    fields = [ref.at[c] for ref in (u_ref, load_ref, weight_ref) for c in range(3)] + [s_ref]
    for f in range(10):
        for z in range(PLANES):
            fields[f][z, :, pl.ds(0, 128)] = ext_ref[f, z]
        for z in list(range(OWN)) + list(range(OWN + 8, PLANES)):
            fields[f][z, :, pl.ds(128, 128)] = blank
    lane = lane_index((ROWS, 128))
    merged = None
    for k, (f, z) in enumerate(fine_places(gz)):
        group = k % 16
        if group == 0:
            merged = jnp.where(lane % 8 < 4, high_ref[k // 16], low_ref[k // 16])
        value = merged if group == 0 else pltpu.roll(merged, 128 - 8 * group, 1)
        fields[f][z, :, pl.ds(128, 128)] = jnp.where((lane < EDGE) | (lane >= 128 - EDGE), value, 0.0)
    clear_work(y_ref, x_ref, hi_ref, q_ref, r_ref)

    for c in range(3):
        for z1 in range(4):
            z = OWN + 2 * z1
            pair_ref[0] = jnp.minimum(
                weight_ref[c, z, :, pl.ds(0, 128)], weight_ref[c, z + 1, :, pl.ds(0, 128)]
            )
            least = jnp.minimum(pair_ref[0, pl.ds(4, 16, 2), :], pair_ref[0, pl.ds(5, 16, 2), :])
            rows_ref[pl.ds(32 * (4 + c) + 16 * (z1 // 2), 16), pl.ds(128 * (z1 % 2), 128)] = least

    for z in range(1, PLANES - 1):
        for t in range(5):
            rows = pl.ds(8 * t, 8)
            s = s_ref[z, rows, :] + s_ref[z - 1, rows, :]
            for part in range(2):
                r_ref[0, z % 6, part, rows, :] = s[:, 128 * part: 128 * part + 128]
        for t in range(5):
            rows = pl.ds(8 * t, 8)
            s = s_ref[z, rows, :] + s_ref[z - 1, rows, :]
            before = [
                r_ref[0, z % 6, part, pl.ds(8 * t - 1, 8), :] if t else pltpu.roll(s[:, 128 * part: 128 * part + 128], 1, 0)
                for part in range(2)
            ]
            s = s + jnp.concatenate(before, 1)
            inverse = box_inverse(s + pltpu.roll(s, 1, 1), KDIAG)
            for c in range(3):
                weight_ref[c, z, rows, :] = weight_ref[c, z, rows, :] * inverse

    sweep = smoother(u_ref, load_ref, weight_ref)
    tiles = range(5)
    work = (y_ref, x_ref, hi_ref, q_ref, r_ref)
    for k in range(2):
        stencil(u_ref, s_ref, sweep, 3 - 2 * gz + k * gz, 10 - k, tiles, *work)

    def remain(z, t, forces):
        rows = pl.ds(8 * t, 8)
        here = pl.ds(0, 128)
        for c in range(3):
            rest = load_ref[c, z, rows, here] - forces[c][:, :128]
            rest_ref[c, z - OWN, rows, :] = jnp.where(weight_ref[c, z, rows, here] > 0, rest, 0.0)

    stencil(u_ref, s_ref, remain, OWN, 8, tiles, *work)

    for c in range(3):
        for z1 in range(4):
            pair_ref[0] = rest_ref[c, 2 * z1] + rest_ref[c, 2 * z1 + 1]
            total = pair_ref[0, pl.ds(4, 16, 2), :] + pair_ref[0, pl.ds(5, 16, 2), :]
            rows_ref[pl.ds(32 * c + 16 * (z1 // 2), 16), pl.ds(128 * (z1 % 2), 128)] = total
    for z1 in range(4):
        z = OWN + 2 * z1
        pair_ref[0] = s_ref[z, :, pl.ds(0, 128)] + s_ref[z + 1, :, pl.ds(0, 128)]
        total = pair_ref[0, pl.ds(4, 16, 2), :] + pair_ref[0, pl.ds(5, 16, 2), :]
        rows_ref[pl.ds(32 * 3 + 16 * (z1 // 2), 16), pl.ds(128 * (z1 % 2), 128)] = total
        box = []
        for k in range(2):
            here = pl.ds(128 * k, 128)
            pair_ref[k] = (s_ref[z - 2, :, here] + s_ref[z - 1, :, here]) + (
                s_ref[z, :, here] + s_ref[z + 1, :, here]
            )
            box.append(
                (pair_ref[k, pl.ds(2, 16, 2), :] + pair_ref[k, pl.ds(3, 16, 2), :])
                + (pair_ref[k, pl.ds(4, 16, 2), :] + pair_ref[k, pl.ds(5, 16, 2), :])
            )
        lane16 = lane_index((16, 128))
        back = jnp.where(lane16 < 2, pltpu.roll(box[1], 2, 1), pltpu.roll(box[0], 2, 1))
        rows_ref[pl.ds(32 * 7 + 16 * (z1 // 2), 16), pl.ds(128 * (z1 % 2), 128)] = box[0] + back

    source = lax.broadcasted_iota(jnp.int32, (256, 128), 0)
    target = lax.broadcasted_iota(jnp.int32, (256, 128), 1)
    join = jnp.where(source // 2 == target, 1.0, 0.0).astype(F32)
    level1 = jnp.dot(rows_ref[...], join, precision=lax.Precision.HIGHEST, preferred_element_type=F32)

    def part(k):
        return level1[32 * k: 32 * k + 32]

    inverse = box_inverse(part(7), 2.0 * KDIAG / 8)
    results = [part(0), part(1), part(2), part(3) * (2.0 / 8)]
    results += [jnp.where(part(4 + c) > 1.5, inverse, 0.0) for c in range(3)]
    for k in range(7):
        for pair in range(2):
            send_ref[k, pair] = results[k][16 * pair: 16 * pair + 16]
    away = OWN + 6 - 5 * gz
    for c in range(3):
        plane_ref[c] = u_ref[c, away]


def edge_rows1(gz_ref, own_ref, other_ref, full_ref, right_ref, left_ref):
    gz = gz_ref[0]
    for f in range(7):
        full_ref[f, pl.ds(2 * gz, 2)] = own_ref[f]
        full_ref[f, pl.ds(2 - 2 * gz, 2)] = other_ref[f]
    for f in range(7):
        for pair in range(4):
            k = 4 * f + pair
            right_ref[pl.ds(12 * k, 12)] = full_ref[f, pair, pl.ds(4, 12)]
            left_ref[pl.ds(12 * k, 12)] = full_ref[f, pair, pl.ds(0, 12)]


def edge_lanes1(gz_ref, full_ref, low_ref, high_ref, ext_ref, right_ref, left_ref):
    lane = lane_index((ROWS, 128))
    for f in range(7):
        right = left = None
        for pair in range(4):
            k = 4 * f + pair
            ext_ref[f, pair, pl.ds(0, 12)] = low_ref[pl.ds(12 * k, 12)]
            ext_ref[f, pair, pl.ds(12, 16)] = full_ref[f, pair]
            ext_ref[f, pair, pl.ds(28, 12)] = high_ref[pl.ds(12 * k, 12)]
            value = ext_ref[f, pair]
            moved = pltpu.roll(value, 16 * pair, 1) if pair else value
            place = (lane + (128 - 16 * pair)) % 64
            right = moved if right is None else jnp.where(place >= 52, moved, right)
            left = moved if left is None else jnp.where(place < 12, moved, left)
        right_ref[f] = right
        left_ref[f] = left


def coarse(gz_ref, ext_ref, low_ref, high_ref, old_ref, load_ref, weight_ref, s_ref, other_ref, out_ref,
           u1_ref, v1_ref, u2_ref, v2_ref, state_ref, rest_ref, rows_ref, pair_ref, *work):
    work, fine_work = work[:5], work[5:]
    gz = gz_ref[0]
    lane = lane_index((ROWS, 128))
    clear_work(*work)
    clear_work(*fine_work)
    clear(u2_ref, v2_ref)
    for f in range(7):
        for z in (0, 9):
            v1_ref[f, z] = jnp.zeros((ROWS, 128), F32)
    for f in range(7):
        low, high = low_ref[f], high_ref[f]
        for pair in range(4):
            value = ext_ref[f, pair]
            for half in range(2):
                own = value if half == 0 else pltpu.roll(value, 64, 1)
                turn = (64 - 16 * pair - 64 * half) % 128
                below = pltpu.roll(low, turn, 1) if turn else low
                above = pltpu.roll(high, turn, 1) if turn else high
                whole = jnp.where(
                    lane < 64, own, jnp.where(lane < 64 + EDGE1, above, jnp.where(lane >= 128 - EDGE1, below, 0.0))
                )
                v1_ref[f, 1 + 2 * pair + half] = whole
    for c in range(3):
        for z in range(10):
            u1_ref[c, z] = v1_ref[4 + c, z] * v1_ref[c, z]

    s1_ref = v1_ref.at[3]
    sweep1 = smoother(u1_ref, v1_ref, v1_ref.at[pl.ds(4, 3)])
    stencil(u1_ref, s1_ref, sweep1, 1, 8, range(5), *work)

    def remain(z, t, forces):
        rows = pl.ds(8 * t, 8)
        for c in range(3):
            rest = v1_ref[c, z, rows, :] - forces[c]
            rest_ref[c, z, rows, :] = jnp.where(v1_ref[4 + c, z, rows, :] > 0, rest, 0.0)

    stencil(u1_ref, s1_ref, remain, 1, 8, range(5), *work)

    for z2 in range(4):
        z = 1 + 2 * z2
        for c in range(3):
            rest_ref[c, z] = rest_ref[c, z] + rest_ref[c, z + 1]
            rows_ref[pl.ds(24 * (4 * c + z2), 20)] = rest_ref[c, z, pl.ds(0, 20, 2), :] + rest_ref[c, z, pl.ds(1, 20, 2), :]
            rest_ref[c, 9] = jnp.where((v1_ref[4 + c, z] > 0) & (v1_ref[4 + c, z + 1] > 0), 1.0, 0.0)
            rows_ref[pl.ds(24 * (16 + 4 * c + z2), 20)] = jnp.minimum(
                rest_ref[c, 9, pl.ds(0, 20, 2), :], rest_ref[c, 9, pl.ds(1, 20, 2), :]
            )
        rest_ref[0, 9] = v1_ref[3, z] + v1_ref[3, z + 1]
        rows_ref[pl.ds(24 * (12 + z2), 20)] = rest_ref[0, 9, pl.ds(0, 20, 2), :] + rest_ref[0, 9, pl.ds(1, 20, 2), :]
    for k in range(28):
        rows_ref[pl.ds(24 * k + 20, 4)] = jnp.zeros((4, 128), F32)
    source = lax.broadcasted_iota(jnp.int32, (128, 128), 0)
    target = lax.broadcasted_iota(jnp.int32, (128, 128), 1)
    used = (target < 40) | (target >= 120)
    fold = (source // 2 + jnp.where(target < 64, 0, 64) == target) & used
    join = jnp.where(fold, 1.0, 0.0).astype(F32)
    level2 = jnp.dot(rows_ref[...], join, precision=lax.Precision.HIGHEST, preferred_element_type=F32)

    def part(k, z2):
        return level2[24 * (4 * k + z2): 24 * (4 * k + z2) + 24]

    for z2 in range(4):
        for c in range(3):
            v2_ref[c, 1 + z2] = part(c, z2)
            v2_ref[4 + c, 1 + z2] = jnp.where(part(4 + c, z2) > 1.5, 1.0, 0.0)
        v2_ref[3, 1 + z2] = part(3, z2) * (4.0 / 2.0 / 8.0)
    for z in range(1, 5):
        for t in range(3):
            rows = pl.ds(8 * t, 8)
            s = v2_ref[3, z, rows, :] + v2_ref[3, z - 1, rows, :]
            if t:
                before = pl.ds(8 * t - 1, 8)
                back = v2_ref[3, z, before, :] + v2_ref[3, z - 1, before, :]
            else:
                back = pltpu.roll(s, 1, 0)
            s = s + back
            inverse = box_inverse(s + pltpu.roll(s, 1, 1), KDIAG)
            for c in range(3):
                weight = v2_ref[4 + c, z, rows, :] * inverse
                v2_ref[4 + c, z, rows, :] = weight
                u2_ref[c, z, rows, :] = weight * v2_ref[c, z, rows, :]

    sweep2 = smoother(u2_ref, v2_ref, v2_ref.at[pl.ds(4, 3)])

    def again(k, carry):
        stencil(u2_ref, v2_ref.at[3], sweep2, 1, 4, range(3), *work)
        return carry

    lax.fori_loop(0, COARSE - 1, again, 0)

    part_of = jnp.where(
        (source == jnp.where(target < 96, target // 2, target // 2 + 64)), 1.0, 0.0
    ).astype(F32)
    for c in range(3):
        for z2 in range(4):
            rows_ref[pl.ds(24 * (4 * c + z2), 24)] = u2_ref[c, 1 + z2]
    spread = jnp.dot(rows_ref[pl.ds(0, 288)], part_of, precision=lax.Precision.HIGHEST, preferred_element_type=F32)
    for c in range(3):
        for z2 in range(4):
            k = 24 * (4 * c + z2)
            value = spread[k: k + 24][:20]
            rest_ref[c, 9, pl.ds(0, 20, 2), :] = value
            rest_ref[c, 9, pl.ds(1, 20, 2), :] = value
            for z in (1 + 2 * z2, 2 + 2 * z2):
                u1_ref[c, z] = u1_ref[c, z] + jnp.where(v1_ref[4 + c, z] > 0, rest_ref[c, 9], 0.0)

    for k in range(2):
        stencil(u1_ref, s1_ref, sweep1, 1 + 2 * gz + k * gz, 6 - k, range(1, 4), *work)

    start = 4 * gz
    for c in range(3):
        for j in range(6):
            rows_ref[pl.ds(24 * (6 * c + j), 24)] = u1_ref[c, start + j, pl.ds(8, 24), :]
    target2 = lax.broadcasted_iota(jnp.int32, (128, 256), 1)
    source2 = lax.broadcasted_iota(jnp.int32, (128, 256), 0)
    copies = jnp.where(source2 == target2 // 2, 1.0, 0.0).astype(F32)
    fine = jnp.dot(rows_ref[pl.ds(0, 432)], copies, precision=lax.Precision.HIGHEST, preferred_element_type=F32)
    for c in range(3):
        for z in range(PLANES):
            state_ref[c, z] = old_ref[c, z]
        state_ref[c, 12 - 11 * gz] = other_ref[c]
        for j in range(6):
            k = 24 * (6 * c + j)
            value = fine[k: k + 24][2:22]
            for k in range(2):
                here = pl.ds(128 * k, 128)
                pair_ref[k, pl.ds(0, 20, 2), :] = value[:, 128 * k: 128 * k + 128]
                pair_ref[k, pl.ds(1, 20, 2), :] = value[:, 128 * k: 128 * k + 128]
                for half in range(2):
                    z = 1 + 2 * j + half
                    state_ref[c, z, :, here] = state_ref[c, z, :, here] + jnp.where(
                        weight_ref[c, z, :, here] > 0, pair_ref[k], 0.0
                    )

    sweep = smoother(state_ref, load_ref, weight_ref)
    for k in range(2):
        stencil(state_ref, s_ref, sweep, 3 - gz + k * gz, 9 - k, range(5), *fine_work)
    for c in range(3):
        for z in range(8):
            out_ref[c, z] = state_ref[c, OWN + z, pl.ds(4, 32), pl.ds(0, 128)]


def up(value, axis):
    return lax.ppermute(value, axis, [(i, i + 1) for i in range(lax.axis_size(axis) - 1)])


def down(value, axis):
    return lax.ppermute(value, axis, [(i + 1, i) for i in range(lax.axis_size(axis) - 1)])


def swap(value):
    return lax.ppermute(value, "gz", [(0, 1), (1, 0)])


def scratch_of(rows, width, planes):
    parts = width // 128
    return [
        pltpu.VMEM((planes + 2, 6, parts, rows + 8, 128), F32),
        pltpu.VMEM((12, parts, rows, 128), F32),
        pltpu.VMEM((12, parts, rows, 128), F32),
        pltpu.VMEM((6, parts, rows + 8, 128), F32),
        pltpu.VMEM((planes + 1, 6, parts, rows, 128), F32),
    ]


def on_device(displacement, load, density_code, fixed_mask):
    gz = lax.axis_index("gz").astype(jnp.int32).reshape(1)
    inputs = [gz, displacement, load, density_code, fixed_mask]
    (zsend,) = call(
        boundary,
        [(24, 32, 128)],
        inputs,
        [
            pltpu.VMEM((3, 3, 32, 128), F32),
            pltpu.VMEM((3, 2, 32, 128), F32),
            pltpu.VMEM((3, 32, 128), jnp.int32),
            pltpu.VMEM((3, 3, 32, 128), jnp.int32),
            pltpu.SemaphoreType.DMA((4,)),
        ],
        inputs="any",
    )
    zrecv = swap(zsend)
    base, right, left = call(prepare, [(10, 8, 32, 128), (320, 128), (320, 128)], inputs, inputs="plain")
    low, high = up(right, "gx"), down(left, "gx")
    (zsend,) = call(boundary_rows, [(192, 128)], [gz, low, high])
    beside = swap(zsend)
    ext, ysend = call(
        edge_lanes, [(10, PLANES, ROWS, 128), (7, ROWS, 128)], [gz, base, zrecv, low, high, beside]
    )
    low, high = up(ysend, "gy"), down(ysend, "gy")
    wide = (3, PLANES, ROWS, LANES)
    u, loads, weights, scales, send1, plane = call(
        fine_down,
        [wide, wide, wide, (PLANES, ROWS, LANES), (7, 2, 16, 128), (3, ROWS, LANES)],
        [gz, ext, low, high],
        scratch_of(ROWS, LANES, 10)
        + [pltpu.VMEM((3, 8, ROWS, 128), F32), pltpu.VMEM((2, ROWS, 128), F32), pltpu.VMEM((256, 256), F32)],
    )
    other1 = swap(send1)
    other_plane = swap(plane)
    full, right, left = call(edge_rows1, [(7, 4, 16, 128), (336, 128), (336, 128)], [gz, send1, other1])
    low, high = up(right, "gx"), down(left, "gx")
    full, low, high, other_plane = lax.optimization_barrier((full, low, high, other_plane))
    ext1, right, left = call(
        edge_lanes1, [(7, 4, ROWS, 128), (7, ROWS, 128), (7, ROWS, 128)], [gz, full, low, high]
    )
    low, high = up(right, "gy"), down(left, "gy")
    (out,) = call(
        coarse,
        [(3, 8, 32, 128)],
        [gz, ext1, low, high, u, loads, weights, scales, other_plane],
        [
            pltpu.VMEM((3, 10, ROWS, 128), F32),
            pltpu.VMEM((7, 10, ROWS, 128), F32),
            pltpu.VMEM((3, 6, 24, 128), F32),
            pltpu.VMEM((7, 6, 24, 128), F32),
            pltpu.VMEM(wide, F32),
            pltpu.VMEM((3, 10, ROWS, 128), F32),
            pltpu.VMEM((672, 128), F32),
            pltpu.VMEM((2, ROWS, 128), F32),
        ]
        + scratch_of(ROWS, 128, 8)
        + scratch_of(ROWS, LANES, 9),
        output="plain",
    )
    return out


def solution(mesh):
    return jax.shard_map(
        on_device,
        mesh=mesh,
        in_specs=(
            P(None, "gz", "gx", "gy"),
            P(None, "gz", "gx", "gy"),
            P("gz", "gx", "gy"),
            P(None, "gz", "gx", "gy"),
        ),
        out_specs=P(None, "gz", "gx", "gy"),
        check_vma=False,
    )
```

```python
import jax
import jax.numpy as jnp
from jax import lax
from jax.experimental import pallas as pl
from jax.experimental.pallas import tpu as pltpu
from jax.sharding import PartitionSpec as P

LEVELS = 16
COARSE = 4
EMIN = 0.001
OMEGA = 0.5

POISSON = 0.3
LAME = POISSON / ((1 + POISSON) * (1 - 2 * POISSON))
SHEAR = 1 / (2 * (1 + POISSON))
KDIAG = (LAME + 4 * SHEAR) / 16 + 2 * (LAME + 3 * SHEAR) / 48 + 2 * SHEAR / 48 + (LAME + 4 * SHEAR) / 144

PLANES, ROWS, LANES = 14, 40, 256
OWN = 3
EDGE = 4
EDGE1 = 12

F32 = jnp.float32


def element(c, s):
    s16l, s16m = s * (LAME / 16), s * (SHEAR / 16)
    s16n = s * (2 * SHEAR / 16)
    s48l, s48m, s48n = s * (LAME / 48), s * (SHEAR / 48), s * ((LAME + 3 * SHEAR) / 48)
    s144 = s * ((LAME + 4 * SHEAR) / 144)

    def at(*dims):
        return tuple(1 if d in dims else 0 for d in range(3))

    g = {}
    trace = s16l * (c[0, at(0)] + c[1, at(1)] + c[2, at(2)])
    for i in range(3):
        g[i, at(i)] = s16n * c[i, at(i)] + trace
    for i, j in ((0, 1), (0, 2), (1, 2)):
        force = s16m * (c[i, at(j)] + c[j, at(i)])
        g[i, at(j)] = force
        g[j, at(i)] = force
    for j in range(3):
        i, k = [d for d in range(3) if d != j]
        first, second = c[i, at(i, j)], c[k, at(k, j)]
        g[i, at(i, j)] = s48n * first + s48l * second
        g[k, at(k, j)] = s48n * second + s48l * first
    twists = [c[i, at(*[d for d in range(3) if d != i])] for i in range(3)]
    total = twists[0] + twists[1] + twists[2]
    for i in range(3):
        g[i, at(*[d for d in range(3) if d != i])] = s48m * (twists[i] + total)
        g[i, (1, 1, 1)] = s144 * c[i, (1, 1, 1)]
    return g


def stencil(u_ref, s_ref, emit, first, count, tiles, y_ref, x_ref, hi_ref, q_ref, r_ref):
    width = u_ref.shape[-1]
    parts = width // 128

    def split(value):
        return [value[:, 128 * part: 128 * part + 128] for part in range(parts)]

    def join(values):
        return jnp.concatenate(values, 1) if parts > 1 else values[0]

    for j in range(count + 2):
        for t in tiles:
            rows = pl.ds(8 * t, 8)
            for c in range(3):
                u = u_ref[c, first - 1 + j, rows, :]
                after = pltpu.roll(u, width - 1, 1)
                for k, value in enumerate((u + after, after - u)):
                    for part, piece in enumerate(split(value)):
                        y_ref[j, 2 * c + k, part, rows, :] = piece

    def spread_x(j, t, part):
        out = []
        for k in range(6):
            here = y_ref[j, k, part, pl.ds(8 * t, 8), :]
            after = y_ref[j, k, part, pl.ds(8 * t + 1, 8), :]
            out += [here + after, after - here]
        return out

    for t in tiles:
        for part in range(parts):
            for i, value in enumerate(spread_x(0, t, part)):
                x_ref[i, part, pl.ds(8 * t, 8), :] = value

    def layer(step, carry):
        e = first - 1 + step
        for t in tiles:
            rows = pl.ds(8 * t, 8)
            for part in range(parts):
                c = {}
                for i, now in enumerate(spread_x(step + 1, t, part)):
                    comp, yt, xt = i // 4, i // 2 % 2, i % 2
                    before = x_ref[i, part, rows, :]
                    x_ref[i, part, rows, :] = now
                    c[comp, (0, xt, yt)] = now + before
                    c[comp, (1, xt, yt)] = now - before
                g = element(c, s_ref[e, rows, pl.ds(128 * part, 128)])
                for comp in range(3):
                    ends = []
                    for yt in range(2):
                        node = []
                        for xt in range(2):
                            i = 4 * comp + 2 * yt + xt
                            d = g[comp, (1, xt, yt)]
                            a = g.get((comp, (0, xt, yt)))
                            low = hi_ref[i, part, rows, :]
                            if a is None:
                                node.append(low - d)
                                hi_ref[i, part, rows, :] = d
                            else:
                                node.append(low + (a - d))
                                hi_ref[i, part, rows, :] = a + d
                        k = 2 * comp + yt
                        q_ref[k, part, pl.ds(8 * t + 1, 8), :] = node[0] + node[1]
                        ends.append(node[0] - node[1] + q_ref[k, part, rows, :])
                    r_ref[step, 2 * comp, part, rows, :] = ends[0] - ends[1]
                    r_ref[step, 2 * comp + 1, part, rows, :] = ends[0] + ends[1]
        return carry

    lax.fori_loop(0, count + 1, layer, 0)

    for j in range(count):
        for t in tiles:
            rows = pl.ds(8 * t, 8)
            forces = []
            for comp in range(3):
                low = join([r_ref[j + 1, 2 * comp, part, rows, :] for part in range(parts)])
                high = join([r_ref[j + 1, 2 * comp + 1, part, rows, :] for part in range(parts)])
                forces.append(low + pltpu.roll(high, 1, 1))
            emit(first + j, t, forces)


def smoother(u_ref, rhs_ref, weight_ref):
    def sweep(z, t, forces):
        rows = pl.ds(8 * t, 8)
        for c in range(3):
            u = u_ref[c, z, rows, :]
            u_ref[c, z, rows, :] = u + weight_ref[c, z, rows, :] * (rhs_ref[c, z, rows, :] - forces[c])

    return sweep


def box_inverse(total, factor):
    positive = total > 0
    return jnp.where(positive, OMEGA / (factor * jnp.where(positive, total, 1.0)), 0.0)


def clear(*refs):
    for ref in refs:
        for k in range(ref.shape[0]):
            ref[k] = jnp.zeros(ref.shape[1:], F32)


def clear_work(y_ref, x_ref, hi_ref, q_ref, r_ref):
    planes, six, parts, rows, _ = y_ref.shape
    for j in range(planes):
        y_ref[j, :, :, pl.ds(rows - 8, 8), :] = jnp.zeros((six, parts, 8, 128), F32)
    clear(hi_ref, q_ref)


def lane_index(shape):
    return lax.broadcasted_iota(jnp.int32, shape, len(shape) - 1)


def call(body, outs, args, scratch=(), inputs="vmem", output="vmem"):
    whole = pl.BlockSpec(memory_space=pltpu.VMEM)
    space = pltpu.VMEM if inputs == "vmem" else pltpu.HBM
    rest = pl.BlockSpec(memory_space=space)
    values = [pltpu.with_memory_space_constraint(value, space) for value in args[1:]]
    shape = pltpu.VMEM if output == "vmem" else jax.ShapeDtypeStruct
    return pl.pallas_call(
        body,
        out_shape=tuple(shape(out, F32) for out in outs),
        in_specs=[pl.BlockSpec(memory_space=pltpu.SMEM)] + [rest] * len(values),
        out_specs=tuple(whole for _ in outs),
        scratch_shapes=list(scratch),
        compiler_params=pltpu.CompilerParams(vmem_limit_bytes=24 * 1024 * 1024),
    )(args[0], *values)


def scale_of(code):
    level = code.astype(F32) / (LEVELS - 1)
    return EMIN + (1.0 - EMIN) * level * level * level


def prepare(gz_ref, disp_hbm, load_hbm, code_hbm, fixed_hbm, send_ref, base_ref, right_ref, left_ref,
            disp_ref, load_ref, code_ref, fixed_ref, sems):
    gz = gz_ref[0]
    copies = []
    for half in range(2):
        planes = pl.ds(4 * half, 4)
        pairs = [(code_hbm.at[planes], code_ref.at[planes])]
        for c in range(3):
            for source, target in ((fixed_hbm, fixed_ref), (disp_hbm, disp_ref), (load_hbm, load_ref)):
                pairs.append((source.at[c, planes], target.at[c, planes]))
        for source, target in pairs:
            copies.append(pltpu.make_async_copy(source, target, sems.at[len(copies)]))
    for copy in copies:
        copy.start()
    for copy in copies:
        copy.wait()
    for z in range(8):
        base_ref[9, z] = scale_of(code_ref[z])
        for c in range(3):
            free = 1.0 - fixed_ref[c, z].astype(F32)
            base_ref[c, z] = free * disp_ref[c, z]
            base_ref[3 + c, z] = load_ref[c, z]
            base_ref[6 + c, z] = free
    three, two = 5 * (1 - gz), 6 * (1 - gz)
    for j in range(3):
        send_ref[21 + j] = base_ref[9, three + j]
        for c in range(3):
            send_ref[3 * c + j] = base_ref[c, three + j]
    for c in range(3):
        for j in range(2):
            send_ref[9 + 2 * c + j] = base_ref[3 + c, two + j]
            send_ref[15 + 2 * c + j] = base_ref[6 + c, two + j]
    for k in range(80):
        right_ref[pl.ds(4 * k, 4)] = base_ref[k // 8, k % 8, pl.ds(28, 4)]
        left_ref[pl.ds(4 * k, 4)] = base_ref[k // 8, k % 8, pl.ds(0, 4)]


def boundary_rows(gz_ref, low_ref, high_ref, send_ref):
    lower = gz_ref[0] == 0

    def send(k, f, below, above):
        for i, ref in enumerate((low_ref, high_ref)):
            first, second = 4 * (8 * f + below), 4 * (8 * f + above)
            send_ref[pl.ds(8 * k + 4 * i, 4)] = jnp.where(lower, ref[pl.ds(first, 4)], ref[pl.ds(second, 4)])

    for j in range(3):
        send(21 + j, 9, 5 + j, j)
        for c in range(3):
            send(3 * c + j, c, 5 + j, j)
    for c in range(3):
        for j in range(2):
            send(9 + 2 * c + j, 3 + c, 6 + j, j)
            send(15 + 2 * c + j, 6 + c, 6 + j, j)


def fine_places(gz):
    places = [(f, OWN + z) for f in range(10) for z in range(8)]
    three, two = 11 * (1 - gz), 11 - 10 * gz
    places += [(c, three + j) for c in range(3) for j in range(3)]
    places += [(3 + c, two + j) for c in range(3) for j in range(2)]
    places += [(6 + c, two + j) for c in range(3) for j in range(2)]
    places += [(9, three + j) for j in range(3)]
    return places


def edge_lanes(gz_ref, base_ref, zrecv_ref, low_ref, high_ref, beside_ref, ext_ref, up_ref, down_ref):
    gz = gz_ref[0]
    blank = jnp.zeros((ROWS, 128), F32)
    for f in range(10):
        for z in list(range(OWN)) + list(range(OWN + 8, PLANES)):
            ext_ref[f, z] = blank
    lane = lane_index((ROWS, 128))
    rising = falling = None
    for k, (f, z) in enumerate(fine_places(gz)):
        beside, other = 8 * (k - 80), 1 - gz
        ext_ref[f, z, pl.ds(0, 4)] = low_ref[pl.ds(4 * k, 4)] if k < 80 else beside_ref[other, pl.ds(beside, 4)]
        ext_ref[f, z, pl.ds(4, 32)] = base_ref[k // 8, k % 8] if k < 80 else zrecv_ref[k - 80]
        ext_ref[f, z, pl.ds(36, 4)] = high_ref[pl.ds(4 * k, 4)] if k < 80 else beside_ref[other, pl.ds(beside + 4, 4)]
        group = k % 32
        moved = pltpu.roll(ext_ref[f, z], (4 * group + 4) % 128, 1)
        if group == 0:
            rising = falling = moved
        else:
            rising = jnp.where(lane // 4 == group, moved, rising)
            falling = jnp.where(lane // 4 == (group + 1) % 32, moved, falling)
        if group == 31 or k == 103:
            up_ref[k // 32] = rising
            down_ref[k // 32] = falling


def fine_down(gz_ref, ext_ref, low_ref, high_ref,
              u_ref, load_ref, weight_ref, s_ref, send_ref,
              y_ref, x_ref, hi_ref, q_ref, r_ref, rest_ref, pair_ref, rows_ref):
    gz = gz_ref[0]
    blank = jnp.zeros((ROWS, 128), F32)
    fields = [ref.at[c] for ref in (u_ref, load_ref, weight_ref) for c in range(3)] + [s_ref]
    for f in range(10):
        for z in range(PLANES):
            fields[f][z, :, pl.ds(0, 128)] = ext_ref[f, z]
        for z in list(range(OWN)) + list(range(OWN + 8, PLANES)):
            fields[f][z, :, pl.ds(128, 128)] = blank
    lane = lane_index((ROWS, 128))
    merged = [None, None]
    for k, (f, z) in enumerate(fine_places(gz)):
        group = k % 32
        if group == 0:
            for odd in range(2):
                merged[odd] = jnp.where(lane // 4 % 2 == odd, low_ref[k // 32], high_ref[k // 32])
        value = pltpu.roll(merged[group % 2], 124 - 4 * group, 1) if group < 31 else merged[1]
        fields[f][z, :, pl.ds(128, 128)] = jnp.where((lane < EDGE) | (lane >= 128 - EDGE), value, 0.0)
    clear_work(y_ref, x_ref, hi_ref, q_ref, r_ref)

    for c in range(3):
        for z1 in range(4):
            z = OWN + 2 * z1
            pair_ref[0] = jnp.minimum(
                weight_ref[c, z, :, pl.ds(0, 128)], weight_ref[c, z + 1, :, pl.ds(0, 128)]
            )
            least = jnp.minimum(pair_ref[0, pl.ds(4, 16, 2), :], pair_ref[0, pl.ds(5, 16, 2), :])
            rows_ref[pl.ds(32 * (4 + c) + 16 * (z1 // 2), 16), pl.ds(128 * (z1 % 2), 128)] = least

    for z in range(1, PLANES - 1):
        for t in range(5):
            rows = pl.ds(8 * t, 8)
            s = s_ref[z, rows, :] + s_ref[z - 1, rows, :]
            for part in range(2):
                r_ref[0, z % 6, part, rows, :] = s[:, 128 * part: 128 * part + 128]
        for t in range(5):
            rows = pl.ds(8 * t, 8)
            s = s_ref[z, rows, :] + s_ref[z - 1, rows, :]
            before = [
                r_ref[0, z % 6, part, pl.ds(8 * t - 1, 8), :] if t else pltpu.roll(s[:, 128 * part: 128 * part + 128], 1, 0)
                for part in range(2)
            ]
            s = s + jnp.concatenate(before, 1)
            inverse = box_inverse(s + pltpu.roll(s, 1, 1), KDIAG)
            for c in range(3):
                weight_ref[c, z, rows, :] = weight_ref[c, z, rows, :] * inverse

    sweep = smoother(u_ref, load_ref, weight_ref)
    tiles = range(5)
    work = (y_ref, x_ref, hi_ref, q_ref, r_ref)
    for k in range(2):
        stencil(u_ref, s_ref, sweep, 3 - 2 * gz + k * gz, 10 - k, tiles, *work)

    def remain(z, t, forces):
        rows = pl.ds(8 * t, 8)
        here = pl.ds(0, 128)
        for c in range(3):
            rest = load_ref[c, z, rows, here] - forces[c][:, :128]
            rest_ref[c, z - OWN, rows, :] = jnp.where(weight_ref[c, z, rows, here] > 0, rest, 0.0)

    stencil(u_ref, s_ref, remain, OWN, 8, tiles, *work)

    for c in range(3):
        for z1 in range(4):
            pair_ref[0] = rest_ref[c, 2 * z1] + rest_ref[c, 2 * z1 + 1]
            total = pair_ref[0, pl.ds(4, 16, 2), :] + pair_ref[0, pl.ds(5, 16, 2), :]
            rows_ref[pl.ds(32 * c + 16 * (z1 // 2), 16), pl.ds(128 * (z1 % 2), 128)] = total
    for z1 in range(4):
        z = OWN + 2 * z1
        pair_ref[0] = s_ref[z, :, pl.ds(0, 128)] + s_ref[z + 1, :, pl.ds(0, 128)]
        total = pair_ref[0, pl.ds(4, 16, 2), :] + pair_ref[0, pl.ds(5, 16, 2), :]
        rows_ref[pl.ds(32 * 3 + 16 * (z1 // 2), 16), pl.ds(128 * (z1 % 2), 128)] = total
        box = []
        for k in range(2):
            here = pl.ds(128 * k, 128)
            pair_ref[k] = (s_ref[z - 2, :, here] + s_ref[z - 1, :, here]) + (
                s_ref[z, :, here] + s_ref[z + 1, :, here]
            )
            box.append(
                (pair_ref[k, pl.ds(2, 16, 2), :] + pair_ref[k, pl.ds(3, 16, 2), :])
                + (pair_ref[k, pl.ds(4, 16, 2), :] + pair_ref[k, pl.ds(5, 16, 2), :])
            )
        lane16 = lane_index((16, 128))
        back = jnp.where(lane16 < 2, pltpu.roll(box[1], 2, 1), pltpu.roll(box[0], 2, 1))
        rows_ref[pl.ds(32 * 7 + 16 * (z1 // 2), 16), pl.ds(128 * (z1 % 2), 128)] = box[0] + back

    source = lax.broadcasted_iota(jnp.int32, (256, 128), 0)
    target = lax.broadcasted_iota(jnp.int32, (256, 128), 1)
    join = jnp.where(source // 2 == target, 1.0, 0.0).astype(F32)
    level1 = jnp.dot(rows_ref[...], join, precision=lax.Precision.HIGHEST, preferred_element_type=F32)

    def part(k):
        return level1[32 * k: 32 * k + 32]

    inverse = box_inverse(part(7), 2.0 * KDIAG / 8)
    results = [part(0), part(1), part(2), part(3) * (2.0 / 8)]
    results += [jnp.where(part(4 + c) > 1.5, inverse, 0.0) for c in range(3)]
    for k in range(7):
        for i in range(4):
            send_ref[4 * k + i] = results[k][8 * i: 8 * i + 8]
    away = OWN + 6 - 5 * gz
    lane8 = lane_index((8, 128))
    for t in range(5):
        rows = pl.ds(8 * t, 8)
        edges = u_ref[0, away, rows, pl.ds(128, 128)]
        for c in range(3):
            send_ref[28 + 5 * c + t] = u_ref[c, away, rows, pl.ds(0, 128)]
            if c:
                moved = pltpu.roll(u_ref[c, away, rows, pl.ds(128, 128)], 8 * c, 1)
                edges = jnp.where((lane8 >= 8 * c - 4) & (lane8 < 8 * c + 4), moved, edges)
        send_ref[43 + t] = edges


def edge_rows1(gz_ref, both_ref, full_ref, right_ref, left_ref):
    for f in range(7):
        for pair in range(4):
            for i in range(2):
                full_ref[f, pair, pl.ds(8 * i, 8)] = both_ref[pair // 2, 4 * f + 2 * (pair % 2) + i]
    for f in range(7):
        for pair in range(4):
            k = 4 * f + pair
            right_ref[pl.ds(12 * k, 12)] = full_ref[f, pair, pl.ds(4, 12)]
            left_ref[pl.ds(12 * k, 12)] = full_ref[f, pair, pl.ds(0, 12)]


def edge_lanes1(gz_ref, full_ref, low_ref, high_ref, ext_ref, right_ref, left_ref):
    lane = lane_index((ROWS, 128))
    for f in range(7):
        right = left = None
        for pair in range(4):
            k = 4 * f + pair
            ext_ref[f, pair, pl.ds(0, 12)] = low_ref[pl.ds(12 * k, 12)]
            ext_ref[f, pair, pl.ds(12, 16)] = full_ref[f, pair]
            ext_ref[f, pair, pl.ds(28, 12)] = high_ref[pl.ds(12 * k, 12)]
            value = ext_ref[f, pair]
            moved = pltpu.roll(value, 16 * pair, 1) if pair else value
            place = (lane + (128 - 16 * pair)) % 64
            right = moved if right is None else jnp.where(place >= 52, moved, right)
            left = moved if left is None else jnp.where(place < 12, moved, left)
        right_ref[f] = right
        left_ref[f] = left


def coarse(gz_ref, ext_ref, low_ref, high_ref, old_ref, load_ref, weight_ref, s_ref, both_ref, out_ref,
           u1_ref, v1_ref, u2_ref, v2_ref, state_ref, rest_ref, rows_ref, pair_ref, *work):
    work, fine_work = work[:5], work[5:]
    gz = gz_ref[0]
    lane = lane_index((ROWS, 128))
    clear_work(*work)
    clear_work(*fine_work)
    clear(u2_ref, v2_ref)
    for f in range(7):
        for z in (0, 9):
            v1_ref[f, z] = jnp.zeros((ROWS, 128), F32)
    for f in range(7):
        low, high = low_ref[f], high_ref[f]
        for pair in range(4):
            value = ext_ref[f, pair]
            for half in range(2):
                own = value if half == 0 else pltpu.roll(value, 64, 1)
                turn = (64 - 16 * pair - 64 * half) % 128
                below = pltpu.roll(low, turn, 1) if turn else low
                above = pltpu.roll(high, turn, 1) if turn else high
                whole = jnp.where(
                    lane < 64, own, jnp.where(lane < 64 + EDGE1, above, jnp.where(lane >= 128 - EDGE1, below, 0.0))
                )
                v1_ref[f, 1 + 2 * pair + half] = whole
    for c in range(3):
        for z in range(10):
            u1_ref[c, z] = v1_ref[4 + c, z] * v1_ref[c, z]

    s1_ref = v1_ref.at[3]
    sweep1 = smoother(u1_ref, v1_ref, v1_ref.at[pl.ds(4, 3)])
    stencil(u1_ref, s1_ref, sweep1, 1, 8, range(5), *work)

    def remain(z, t, forces):
        rows = pl.ds(8 * t, 8)
        for c in range(3):
            rest = v1_ref[c, z, rows, :] - forces[c]
            rest_ref[c, z, rows, :] = jnp.where(v1_ref[4 + c, z, rows, :] > 0, rest, 0.0)

    stencil(u1_ref, s1_ref, remain, 1, 8, range(5), *work)

    for z2 in range(4):
        z = 1 + 2 * z2
        for c in range(3):
            rest_ref[c, z] = rest_ref[c, z] + rest_ref[c, z + 1]
            rows_ref[pl.ds(24 * (4 * c + z2), 20)] = rest_ref[c, z, pl.ds(0, 20, 2), :] + rest_ref[c, z, pl.ds(1, 20, 2), :]
            rest_ref[c, 9] = jnp.where((v1_ref[4 + c, z] > 0) & (v1_ref[4 + c, z + 1] > 0), 1.0, 0.0)
            rows_ref[pl.ds(24 * (16 + 4 * c + z2), 20)] = jnp.minimum(
                rest_ref[c, 9, pl.ds(0, 20, 2), :], rest_ref[c, 9, pl.ds(1, 20, 2), :]
            )
        rest_ref[0, 9] = v1_ref[3, z] + v1_ref[3, z + 1]
        rows_ref[pl.ds(24 * (12 + z2), 20)] = rest_ref[0, 9, pl.ds(0, 20, 2), :] + rest_ref[0, 9, pl.ds(1, 20, 2), :]
    for k in range(28):
        rows_ref[pl.ds(24 * k + 20, 4)] = jnp.zeros((4, 128), F32)
    source = lax.broadcasted_iota(jnp.int32, (128, 128), 0)
    target = lax.broadcasted_iota(jnp.int32, (128, 128), 1)
    used = (target < 40) | (target >= 120)
    fold = (source // 2 + jnp.where(target < 64, 0, 64) == target) & used
    join = jnp.where(fold, 1.0, 0.0).astype(F32)
    level2 = jnp.dot(rows_ref[...], join, precision=lax.Precision.HIGHEST, preferred_element_type=F32)

    def part(k, z2):
        return level2[24 * (4 * k + z2): 24 * (4 * k + z2) + 24]

    for z2 in range(4):
        for c in range(3):
            v2_ref[c, 1 + z2] = part(c, z2)
            v2_ref[4 + c, 1 + z2] = jnp.where(part(4 + c, z2) > 1.5, 1.0, 0.0)
        v2_ref[3, 1 + z2] = part(3, z2) * (4.0 / 2.0 / 8.0)
    for z in range(1, 5):
        for t in range(3):
            rows = pl.ds(8 * t, 8)
            s = v2_ref[3, z, rows, :] + v2_ref[3, z - 1, rows, :]
            if t:
                before = pl.ds(8 * t - 1, 8)
                back = v2_ref[3, z, before, :] + v2_ref[3, z - 1, before, :]
            else:
                back = pltpu.roll(s, 1, 0)
            s = s + back
            inverse = box_inverse(s + pltpu.roll(s, 1, 1), KDIAG)
            for c in range(3):
                weight = v2_ref[4 + c, z, rows, :] * inverse
                v2_ref[4 + c, z, rows, :] = weight
                u2_ref[c, z, rows, :] = weight * v2_ref[c, z, rows, :]

    sweep2 = smoother(u2_ref, v2_ref, v2_ref.at[pl.ds(4, 3)])

    def again(k, carry):
        stencil(u2_ref, v2_ref.at[3], sweep2, 1, 4, range(3), *work)
        return carry

    lax.fori_loop(0, COARSE - 1, again, 0)

    part_of = jnp.where(
        (source == jnp.where(target < 96, target // 2, target // 2 + 64)), 1.0, 0.0
    ).astype(F32)
    for c in range(3):
        for z2 in range(4):
            rows_ref[pl.ds(24 * (4 * c + z2), 24)] = u2_ref[c, 1 + z2]
    spread = jnp.dot(rows_ref[pl.ds(0, 288)], part_of, precision=lax.Precision.HIGHEST, preferred_element_type=F32)
    for c in range(3):
        for z2 in range(4):
            k = 24 * (4 * c + z2)
            value = spread[k: k + 24][:20]
            rest_ref[c, 9, pl.ds(0, 20, 2), :] = value
            rest_ref[c, 9, pl.ds(1, 20, 2), :] = value
            for z in (1 + 2 * z2, 2 + 2 * z2):
                u1_ref[c, z] = u1_ref[c, z] + jnp.where(v1_ref[4 + c, z] > 0, rest_ref[c, 9], 0.0)

    for k in range(2):
        stencil(u1_ref, s1_ref, sweep1, 1 + 2 * gz + k * gz, 6 - k, range(1, 4), *work)

    start = 4 * gz
    lane8 = lane_index((8, 128))
    for c in range(3):
        for j in range(6):
            rows_ref[pl.ds(24 * (6 * c + j), 24)] = u1_ref[c, start + j, pl.ds(8, 24), :]
    target2 = lax.broadcasted_iota(jnp.int32, (128, 256), 1)
    source2 = lax.broadcasted_iota(jnp.int32, (128, 256), 0)
    copies = jnp.where(source2 == target2 // 2, 1.0, 0.0).astype(F32)
    fine = jnp.dot(rows_ref[pl.ds(0, 432)], copies, precision=lax.Precision.HIGHEST, preferred_element_type=F32)
    for c in range(3):
        for z in range(1, PLANES - 1):
            state_ref[c, z] = old_ref[c, z]
        for t in range(5):
            edges = both_ref[1 - gz, 43 + t]
            edges = pltpu.roll(edges, 128 - 8 * c, 1) if c else edges
            edges = jnp.where((lane8 < 4) | (lane8 >= 124), edges, 0.0)
            state_ref[c, 12 - 11 * gz, pl.ds(8 * t, 8), pl.ds(0, 128)] = both_ref[1 - gz, 28 + 5 * c + t]
            state_ref[c, 12 - 11 * gz, pl.ds(8 * t, 8), pl.ds(128, 128)] = edges
        for j in range(6):
            k = 24 * (6 * c + j)
            value = fine[k: k + 24][2:22]
            for k in range(2):
                here = pl.ds(128 * k, 128)
                pair_ref[k, pl.ds(0, 20, 2), :] = value[:, 128 * k: 128 * k + 128]
                pair_ref[k, pl.ds(1, 20, 2), :] = value[:, 128 * k: 128 * k + 128]
                for half in range(2):
                    z = 1 + 2 * j + half
                    state_ref[c, z, :, here] = state_ref[c, z, :, here] + jnp.where(
                        weight_ref[c, z, :, here] > 0, pair_ref[k], 0.0
                    )

    sweep = smoother(state_ref, load_ref, weight_ref)
    for k in range(2):
        stencil(state_ref, s_ref, sweep, 3 - gz + k * gz, 9 - k, range(5), *fine_work)
    for c in range(3):
        for z in range(8):
            out_ref[c, z] = state_ref[c, OWN + z, pl.ds(4, 32), pl.ds(0, 128)]


def up(value, axis):
    return lax.ppermute(value, axis, [(i, i + 1) for i in range(lax.axis_size(axis) - 1)])


def down(value, axis):
    return lax.ppermute(value, axis, [(i + 1, i) for i in range(lax.axis_size(axis) - 1)])


def swap(value):
    return lax.ppermute(value, "gz", [(0, 1), (1, 0)])


def scratch_of(rows, width, planes):
    parts = width // 128
    return [
        pltpu.VMEM((planes + 2, 6, parts, rows + 8, 128), F32),
        pltpu.VMEM((12, parts, rows, 128), F32),
        pltpu.VMEM((12, parts, rows, 128), F32),
        pltpu.VMEM((6, parts, rows + 8, 128), F32),
        pltpu.VMEM((planes + 1, 6, parts, rows, 128), F32),
    ]


def on_device(displacement, load, density_code, fixed_mask):
    gz = lax.axis_index("gz").astype(jnp.int32).reshape(1)
    block = (3, 8, 32, 128)
    zsend, base, right, left = call(
        prepare,
        [(24, 32, 128), (10, 8, 32, 128), (320, 128), (320, 128)],
        [gz, displacement, load, density_code, fixed_mask],
        [
            pltpu.VMEM(block, F32),
            pltpu.VMEM(block, F32),
            pltpu.VMEM(block[1:], jnp.int32),
            pltpu.VMEM(block, jnp.int32),
            pltpu.SemaphoreType.DMA((20,)),
        ],
        inputs="hbm",
    )
    zrecv = swap(zsend)
    low, high = up(right, "gx"), down(left, "gx")
    (zsend,) = call(boundary_rows, [(192, 128)], [gz, low, high])
    beside = lax.all_gather(zsend, "gz")
    ext, rising, falling = call(
        edge_lanes,
        [(10, PLANES, ROWS, 128), (4, ROWS, 128), (4, ROWS, 128)],
        [gz, base, zrecv, low, high, beside],
    )
    low, high = up(rising, "gy"), down(falling, "gy")
    wide = (3, PLANES, ROWS, LANES)
    u, loads, weights, scales, send1 = call(
        fine_down,
        [wide, wide, wide, (PLANES, ROWS, LANES), (48, 8, 128)],
        [gz, ext, low, high],
        scratch_of(ROWS, LANES, 10)
        + [pltpu.VMEM((3, 8, ROWS, 128), F32), pltpu.VMEM((2, ROWS, 128), F32), pltpu.VMEM((256, 256), F32)],
    )
    both = lax.all_gather(send1, "gz")
    full, right, left = call(edge_rows1, [(7, 4, 16, 128), (336, 128), (336, 128)], [gz, both])
    low, high = up(right, "gx"), down(left, "gx")
    ext1, right, left = call(
        edge_lanes1, [(7, 4, ROWS, 128), (7, ROWS, 128), (7, ROWS, 128)], [gz, full, low, high]
    )
    low, high = up(right, "gy"), down(left, "gy")
    (out,) = call(
        coarse,
        [(3, 8, 32, 128)],
        [gz, ext1, low, high, u, loads, weights, scales, both],
        [
            pltpu.VMEM((3, 10, ROWS, 128), F32),
            pltpu.VMEM((7, 10, ROWS, 128), F32),
            pltpu.VMEM((3, 6, 24, 128), F32),
            pltpu.VMEM((7, 6, 24, 128), F32),
            pltpu.VMEM(wide, F32),
            pltpu.VMEM((3, 10, ROWS, 128), F32),
            pltpu.VMEM((672, 128), F32),
            pltpu.VMEM((2, ROWS, 128), F32),
        ]
        + scratch_of(ROWS, 128, 8)
        + scratch_of(ROWS, LANES, 9),
        output="plain",
    )
    return out


def solution(mesh):
    return jax.shard_map(
        on_device,
        mesh=mesh,
        in_specs=(
            P(None, "gz", "gx", "gy"),
            P(None, "gz", "gx", "gy"),
            P("gz", "gx", "gy"),
            P(None, "gz", "gx", "gy"),
        ),
        out_specs=P(None, "gz", "gx", "gy"),
        check_vma=False,
    )
```

```python
import jax
import jax.numpy as jnp
from jax import lax
from jax.experimental import pallas as pl
from jax.experimental.pallas import tpu as pltpu
from jax.sharding import PartitionSpec as P

LEVELS = 16
COARSE = 4
EMIN = 0.001
OMEGA = 0.5

POISSON = 0.3
LAME = POISSON / ((1 + POISSON) * (1 - 2 * POISSON))
SHEAR = 1 / (2 * (1 + POISSON))
KDIAG = (LAME + 4 * SHEAR) / 16 + 2 * (LAME + 3 * SHEAR) / 48 + 2 * SHEAR / 48 + (LAME + 4 * SHEAR) / 144

PLANES, ROWS, LANES = 14, 40, 256
OWN = 3
EDGE = 4
EDGE1 = 12

F32 = jnp.float32


def element(c, s):
    s16l, s16m = s * (LAME / 16), s * (SHEAR / 16)
    s16n = s * (2 * SHEAR / 16)
    s48l, s48m, s48n = s * (LAME / 48), s * (SHEAR / 48), s * ((LAME + 3 * SHEAR) / 48)
    s144 = s * ((LAME + 4 * SHEAR) / 144)

    def at(*dims):
        return tuple(1 if d in dims else 0 for d in range(3))

    g = {}
    trace = s16l * (c[0, at(0)] + c[1, at(1)] + c[2, at(2)])
    for i in range(3):
        g[i, at(i)] = s16n * c[i, at(i)] + trace
    for i, j in ((0, 1), (0, 2), (1, 2)):
        force = s16m * (c[i, at(j)] + c[j, at(i)])
        g[i, at(j)] = force
        g[j, at(i)] = force
    for j in range(3):
        i, k = [d for d in range(3) if d != j]
        first, second = c[i, at(i, j)], c[k, at(k, j)]
        g[i, at(i, j)] = s48n * first + s48l * second
        g[k, at(k, j)] = s48n * second + s48l * first
    twists = [c[i, at(*[d for d in range(3) if d != i])] for i in range(3)]
    total = twists[0] + twists[1] + twists[2]
    for i in range(3):
        g[i, at(*[d for d in range(3) if d != i])] = s48m * (twists[i] + total)
        g[i, (1, 1, 1)] = s144 * c[i, (1, 1, 1)]
    return g


def stencil(u_ref, s_ref, emit, first, count, tiles, y_ref, x_ref, hi_ref, q_ref, r_ref):
    width = u_ref.shape[-1]
    parts = width // 128

    def split(value):
        return [value[:, 128 * part: 128 * part + 128] for part in range(parts)]

    def join(values):
        return jnp.concatenate(values, 1) if parts > 1 else values[0]

    for j in range(count + 2):
        for t in tiles:
            rows = pl.ds(8 * t, 8)
            for c in range(3):
                u = u_ref[c, first - 1 + j, rows, :]
                after = pltpu.roll(u, width - 1, 1)
                for k, value in enumerate((u + after, after - u)):
                    for part, piece in enumerate(split(value)):
                        y_ref[j, 2 * c + k, part, rows, :] = piece

    def spread_x(j, t, part):
        out = []
        for k in range(6):
            here = y_ref[j, k, part, pl.ds(8 * t, 8), :]
            after = y_ref[j, k, part, pl.ds(8 * t + 1, 8), :]
            out += [here + after, after - here]
        return out

    for t in tiles:
        for part in range(parts):
            for i, value in enumerate(spread_x(0, t, part)):
                x_ref[i, part, pl.ds(8 * t, 8), :] = value

    def layer(step, carry):
        e = first - 1 + step
        for t in tiles:
            rows = pl.ds(8 * t, 8)
            for part in range(parts):
                c = {}
                for i, now in enumerate(spread_x(step + 1, t, part)):
                    comp, yt, xt = i // 4, i // 2 % 2, i % 2
                    before = x_ref[i, part, rows, :]
                    x_ref[i, part, rows, :] = now
                    c[comp, (0, xt, yt)] = now + before
                    c[comp, (1, xt, yt)] = now - before
                g = element(c, s_ref[e, rows, pl.ds(128 * part, 128)])
                for comp in range(3):
                    ends = []
                    for yt in range(2):
                        node = []
                        for xt in range(2):
                            i = 4 * comp + 2 * yt + xt
                            d = g[comp, (1, xt, yt)]
                            a = g.get((comp, (0, xt, yt)))
                            low = hi_ref[i, part, rows, :]
                            if a is None:
                                node.append(low - d)
                                hi_ref[i, part, rows, :] = d
                            else:
                                node.append(low + (a - d))
                                hi_ref[i, part, rows, :] = a + d
                        k = 2 * comp + yt
                        q_ref[k, part, pl.ds(8 * t + 1, 8), :] = node[0] + node[1]
                        ends.append(node[0] - node[1] + q_ref[k, part, rows, :])
                    r_ref[step, 2 * comp, part, rows, :] = ends[0] - ends[1]
                    r_ref[step, 2 * comp + 1, part, rows, :] = ends[0] + ends[1]
        return carry

    lax.fori_loop(0, count + 1, layer, 0)

    for j in range(count):
        for t in tiles:
            rows = pl.ds(8 * t, 8)
            forces = []
            for comp in range(3):
                low = join([r_ref[j + 1, 2 * comp, part, rows, :] for part in range(parts)])
                high = join([r_ref[j + 1, 2 * comp + 1, part, rows, :] for part in range(parts)])
                forces.append(low + pltpu.roll(high, 1, 1))
            emit(first + j, t, forces)


def smoother(u_ref, rhs_ref, weight_ref):
    def sweep(z, t, forces):
        rows = pl.ds(8 * t, 8)
        for c in range(3):
            u = u_ref[c, z, rows, :]
            u_ref[c, z, rows, :] = u + weight_ref[c, z, rows, :] * (rhs_ref[c, z, rows, :] - forces[c])

    return sweep


def box_inverse(total, factor):
    positive = total > 0
    return jnp.where(positive, OMEGA / (factor * jnp.where(positive, total, 1.0)), 0.0)


def clear(*refs):
    for ref in refs:
        for k in range(ref.shape[0]):
            ref[k] = jnp.zeros(ref.shape[1:], F32)


def clear_work(y_ref, x_ref, hi_ref, q_ref, r_ref):
    planes, six, parts, rows, _ = y_ref.shape
    for j in range(planes):
        y_ref[j, :, :, pl.ds(rows - 8, 8), :] = jnp.zeros((six, parts, 8, 128), F32)
    clear(hi_ref, q_ref)


def lane_index(shape):
    return lax.broadcasted_iota(jnp.int32, shape, len(shape) - 1)


def call(body, outs, args, scratch=(), inputs="vmem", output="vmem"):
    whole = pl.BlockSpec(memory_space=pltpu.VMEM)
    space = pltpu.VMEM if inputs == "vmem" else pltpu.HBM
    rest = pl.BlockSpec(memory_space=space)
    values = [pltpu.with_memory_space_constraint(value, space) for value in args[1:]]
    shape = pltpu.VMEM if output == "vmem" else jax.ShapeDtypeStruct
    return pl.pallas_call(
        body,
        out_shape=tuple(shape(out, F32) for out in outs),
        in_specs=[pl.BlockSpec(memory_space=pltpu.SMEM)] + [rest] * len(values),
        out_specs=tuple(whole for _ in outs),
        scratch_shapes=list(scratch),
        compiler_params=pltpu.CompilerParams(vmem_limit_bytes=24 * 1024 * 1024),
    )(args[0], *values)


def scale_of(code):
    level = code.astype(F32) / (LEVELS - 1)
    return EMIN + (1.0 - EMIN) * level * level * level


def prepare(gz_ref, disp_hbm, load_hbm, code_hbm, fixed_hbm, send_ref, base_ref, right_ref, left_ref,
            disp_ref, load_ref, code_ref, fixed_ref, sems):
    gz = gz_ref[0]
    copies = []
    for half in range(2):
        planes = pl.ds(4 * half, 4)
        pairs = [(code_hbm.at[planes], code_ref.at[planes])]
        for c in range(3):
            for source, target in ((fixed_hbm, fixed_ref), (disp_hbm, disp_ref), (load_hbm, load_ref)):
                pairs.append((source.at[c, planes], target.at[c, planes]))
        for source, target in pairs:
            copies.append(pltpu.make_async_copy(source, target, sems.at[len(copies)]))
    for copy in copies:
        copy.start()
    for copy in copies:
        copy.wait()
    for z in range(8):
        base_ref[9, z] = scale_of(code_ref[z])
        for c in range(3):
            free = 1.0 - fixed_ref[c, z].astype(F32)
            base_ref[c, z] = free * disp_ref[c, z]
            base_ref[3 + c, z] = load_ref[c, z]
            base_ref[6 + c, z] = free
    three, two = 5 * (1 - gz), 6 * (1 - gz)
    for j in range(3):
        send_ref[21 + j] = base_ref[9, three + j]
        for c in range(3):
            send_ref[3 * c + j] = base_ref[c, three + j]
    for c in range(3):
        for j in range(2):
            send_ref[9 + 2 * c + j] = base_ref[3 + c, two + j]
            send_ref[15 + 2 * c + j] = base_ref[6 + c, two + j]
    for k in range(80):
        right_ref[pl.ds(4 * k, 4)] = base_ref[k // 8, k % 8, pl.ds(28, 4)]
        left_ref[pl.ds(4 * k, 4)] = base_ref[k // 8, k % 8, pl.ds(0, 4)]


def boundary_rows(gz_ref, low_ref, high_ref, send_ref):
    lower = gz_ref[0] == 0

    def send(k, f, below, above):
        for i, ref in enumerate((low_ref, high_ref)):
            first, second = 4 * (8 * f + below), 4 * (8 * f + above)
            send_ref[pl.ds(8 * k + 4 * i, 4)] = jnp.where(lower, ref[pl.ds(first, 4)], ref[pl.ds(second, 4)])

    for j in range(3):
        send(21 + j, 9, 5 + j, j)
        for c in range(3):
            send(3 * c + j, c, 5 + j, j)
    for c in range(3):
        for j in range(2):
            send(9 + 2 * c + j, 3 + c, 6 + j, j)
            send(15 + 2 * c + j, 6 + c, 6 + j, j)


def fine_places(gz):
    places = [(f, OWN + z) for f in range(10) for z in range(8)]
    three, two = 11 * (1 - gz), 11 - 10 * gz
    places += [(c, three + j) for c in range(3) for j in range(3)]
    places += [(3 + c, two + j) for c in range(3) for j in range(2)]
    places += [(6 + c, two + j) for c in range(3) for j in range(2)]
    places += [(9, three + j) for j in range(3)]
    return places


def edge_lanes(gz_ref, base_ref, zrecv_ref, low_ref, high_ref, beside_ref, ext_ref, up_ref, down_ref):
    gz = gz_ref[0]
    blank = jnp.zeros((ROWS, 128), F32)
    for f in range(10):
        for z in list(range(OWN)) + list(range(OWN + 8, PLANES)):
            ext_ref[f, z] = blank
    lane = lane_index((ROWS, 128))
    rising = falling = None
    for k, (f, z) in enumerate(fine_places(gz)):
        beside, other = 8 * (k - 80), 1 - gz
        ext_ref[f, z, pl.ds(0, 4)] = low_ref[pl.ds(4 * k, 4)] if k < 80 else beside_ref[other, pl.ds(beside, 4)]
        ext_ref[f, z, pl.ds(4, 32)] = base_ref[k // 8, k % 8] if k < 80 else zrecv_ref[k - 80]
        ext_ref[f, z, pl.ds(36, 4)] = high_ref[pl.ds(4 * k, 4)] if k < 80 else beside_ref[other, pl.ds(beside + 4, 4)]
        group = k % 32
        moved = pltpu.roll(ext_ref[f, z], (4 * group + 4) % 128, 1)
        if group == 0:
            rising = falling = moved
        else:
            rising = jnp.where(lane // 4 == group, moved, rising)
            falling = jnp.where(lane // 4 == (group + 1) % 32, moved, falling)
        if group == 31 or k == 103:
            up_ref[k // 32] = rising
            down_ref[k // 32] = falling


def weigh(s_ref, weight_ref, planes, tiles):
    for z in planes:
        for t in tiles:
            rows = pl.ds(8 * t, 8)
            s = s_ref[z, rows, :] + s_ref[z - 1, rows, :]
            if t:
                before = pl.ds(8 * t - 1, 8)
                back = s_ref[z, before, :] + s_ref[z - 1, before, :]
            else:
                back = pltpu.roll(s, 1, 0)
            s = s + back
            inverse = box_inverse(s + pltpu.roll(s, 1, 1), KDIAG)
            for c in range(3):
                weight_ref[c, z, rows, :] = weight_ref[c, z, rows, :] * inverse


def down_stroke(gz, u_ref, load_ref, weight_ref, s_ref, rest_ref, work):
    clear_work(*work)
    weigh(s_ref, weight_ref, range(1, PLANES - 1), range(5))
    sweep = smoother(u_ref, load_ref, weight_ref)
    for k in range(2):
        stencil(u_ref, s_ref, sweep, 3 - 2 * gz + k * gz, 10 - k, range(5), *work)

    def remain(z, t, forces):
        rows = pl.ds(8 * t, 8)
        for c in range(3):
            rest = load_ref[c, z, rows, :] - forces[c]
            rest_ref[c, z - OWN, rows, :] = jnp.where(weight_ref[c, z, rows, :] > 0, rest, 0.0)

    stencil(u_ref, s_ref, remain, OWN, 8, range(5), *work)


def fine_main(gz_ref, ext_ref, u_ref, weight_ref, rest_ref, *work):
    for z in range(PLANES):
        for c in range(3):
            u_ref[c, z] = ext_ref[c, z]
            weight_ref[c, z] = ext_ref[6 + c, z]
    down_stroke(gz_ref[0], u_ref, ext_ref.at[pl.ds(3, 3)], weight_ref, ext_ref.at[9], rest_ref, work)


def fine_edges(gz_ref, ext_ref, low_ref, high_ref, main_u_ref, main_weight_ref, main_rest_ref,
               u_ref, load_ref, weight_ref, s_ref, send_ref,
               strip_u_ref, strip_load_ref, strip_weight_ref, strip_s_ref, strip_rest_ref,
               rest_ref, pair_ref, rows_ref, halo_ref, *work):
    gz = gz_ref[0]
    blank = jnp.zeros((ROWS, 128), F32)
    halos = {3: load_ref.at[0], 4: load_ref.at[1], 5: load_ref.at[2], 9: s_ref}
    outer = list(range(OWN)) + list(range(OWN + 8, PLANES))
    strips = [ref.at[c] for ref in (strip_u_ref, strip_load_ref, strip_weight_ref) for c in range(3)] + [strip_s_ref]
    for f in range(10):
        for z in outer:
            strips[f][z] = blank
    for f, ref in halos.items():
        for z in range(PLANES):
            ref[z, :, pl.ds(0, 128)] = ext_ref[f, z]
        for z in outer:
            ref[z, :, pl.ds(128, 128)] = blank
    lane = lane_index((ROWS, 128))
    left = (lane >= 60) & (lane < 72)
    right = (lane < EDGE) | (lane >= 120)
    merged = [None, None]
    for k, (f, z) in enumerate(fine_places(gz)):
        group = k % 32
        if group == 0:
            for odd in range(2):
                merged[odd] = jnp.where(lane // 4 % 2 == odd, low_ref[k // 32], high_ref[k // 32])
        halo_ref[k] = pltpu.roll(merged[group % 2], 124 - 4 * group, 1) if group < 31 else merged[1]
    for k, (f, z) in enumerate(fine_places(gz)):
        halo = halo_ref[k]
        own = ext_ref[f, z]
        turned = pltpu.roll(jnp.where(lane < 8, own, halo), 64, 1)
        straight = jnp.where(lane < EDGE, halo, own)
        strips[f][z] = jnp.where(left, turned, jnp.where(right, straight, 0.0))
        if f in halos:
            halos[f][z, :, pl.ds(128, 128)] = jnp.where((lane < EDGE) | (lane >= 128 - EDGE), halo, 0.0)

    for c in range(3):
        for z1 in range(4):
            z = OWN + 2 * z1
            pair_ref[0] = jnp.minimum(
                ext_ref[6 + c, z], ext_ref[6 + c, z + 1]
            )
            least = jnp.minimum(pair_ref[0, pl.ds(4, 16, 2), :], pair_ref[0, pl.ds(5, 16, 2), :])
            rows_ref[pl.ds(32 * (4 + c) + 16 * (z1 // 2), 16), pl.ds(128 * (z1 % 2), 128)] = least

    down_stroke(gz, strip_u_ref, strip_load_ref, strip_weight_ref, strip_s_ref, strip_rest_ref, work)

    below, above = lane < EDGE, lane >= 128 - EDGE
    for c in range(3):
        for z in range(1, PLANES - 1):
            for out_ref, main, strip in (
                (u_ref, main_u_ref[c, z], strip_u_ref[c, z]),
                (weight_ref, main_weight_ref[c, z], strip_weight_ref[c, z]),
            ):
                turned = pltpu.roll(strip, 64, 1)
                out_ref[c, z, :, pl.ds(0, 128)] = jnp.where(below, turned, jnp.where(above, strip, main))
                out_ref[c, z, :, pl.ds(128, 128)] = jnp.where(below, strip, jnp.where(above, turned, 0.0))
        for z in range(8):
            strip = strip_rest_ref[c, z]
            turned = pltpu.roll(strip, 64, 1)
            rest_ref[c, z] = jnp.where(below, turned, jnp.where(above, strip, main_rest_ref[c, z]))

    for c in range(3):
        for z1 in range(4):
            pair_ref[0] = rest_ref[c, 2 * z1] + rest_ref[c, 2 * z1 + 1]
            total = pair_ref[0, pl.ds(4, 16, 2), :] + pair_ref[0, pl.ds(5, 16, 2), :]
            rows_ref[pl.ds(32 * c + 16 * (z1 // 2), 16), pl.ds(128 * (z1 % 2), 128)] = total
    for z1 in range(4):
        z = OWN + 2 * z1
        pair_ref[0] = s_ref[z, :, pl.ds(0, 128)] + s_ref[z + 1, :, pl.ds(0, 128)]
        total = pair_ref[0, pl.ds(4, 16, 2), :] + pair_ref[0, pl.ds(5, 16, 2), :]
        rows_ref[pl.ds(32 * 3 + 16 * (z1 // 2), 16), pl.ds(128 * (z1 % 2), 128)] = total
        box = []
        for k in range(2):
            here = pl.ds(128 * k, 128)
            pair_ref[k] = (s_ref[z - 2, :, here] + s_ref[z - 1, :, here]) + (
                s_ref[z, :, here] + s_ref[z + 1, :, here]
            )
            box.append(
                (pair_ref[k, pl.ds(2, 16, 2), :] + pair_ref[k, pl.ds(3, 16, 2), :])
                + (pair_ref[k, pl.ds(4, 16, 2), :] + pair_ref[k, pl.ds(5, 16, 2), :])
            )
        lane16 = lane_index((16, 128))
        back = jnp.where(lane16 < 2, pltpu.roll(box[1], 2, 1), pltpu.roll(box[0], 2, 1))
        rows_ref[pl.ds(32 * 7 + 16 * (z1 // 2), 16), pl.ds(128 * (z1 % 2), 128)] = box[0] + back

    source = lax.broadcasted_iota(jnp.int32, (256, 128), 0)
    target = lax.broadcasted_iota(jnp.int32, (256, 128), 1)
    join = jnp.where(source // 2 == target, 1.0, 0.0).astype(F32)
    level1 = jnp.dot(rows_ref[...], join, precision=lax.Precision.HIGHEST, preferred_element_type=F32)

    def part(k):
        return level1[32 * k: 32 * k + 32]

    inverse = box_inverse(part(7), 2.0 * KDIAG / 8)
    results = [part(0), part(1), part(2), part(3) * (2.0 / 8)]
    results += [jnp.where(part(4 + c) > 1.5, inverse, 0.0) for c in range(3)]
    for k in range(7):
        for i in range(4):
            send_ref[4 * k + i] = results[k][8 * i: 8 * i + 8]
    away = OWN + 6 - 5 * gz
    lane8 = lane_index((8, 128))
    for t in range(5):
        rows = pl.ds(8 * t, 8)
        edges = u_ref[0, away, rows, pl.ds(128, 128)]
        for c in range(3):
            send_ref[28 + 5 * c + t] = u_ref[c, away, rows, pl.ds(0, 128)]
            if c:
                moved = pltpu.roll(u_ref[c, away, rows, pl.ds(128, 128)], 8 * c, 1)
                edges = jnp.where((lane8 >= 8 * c - 4) & (lane8 < 8 * c + 4), moved, edges)
        send_ref[43 + t] = edges


def edge_rows1(gz_ref, both_ref, full_ref, right_ref, left_ref):
    for f in range(7):
        for pair in range(4):
            for i in range(2):
                full_ref[f, pair, pl.ds(8 * i, 8)] = both_ref[pair // 2, 4 * f + 2 * (pair % 2) + i]
    for f in range(7):
        for pair in range(4):
            k = 4 * f + pair
            right_ref[pl.ds(12 * k, 12)] = full_ref[f, pair, pl.ds(4, 12)]
            left_ref[pl.ds(12 * k, 12)] = full_ref[f, pair, pl.ds(0, 12)]


def edge_lanes1(gz_ref, full_ref, low_ref, high_ref, ext_ref, right_ref, left_ref):
    lane = lane_index((ROWS, 128))
    for f in range(7):
        right = left = None
        for pair in range(4):
            k = 4 * f + pair
            ext_ref[f, pair, pl.ds(0, 12)] = low_ref[pl.ds(12 * k, 12)]
            ext_ref[f, pair, pl.ds(12, 16)] = full_ref[f, pair]
            ext_ref[f, pair, pl.ds(28, 12)] = high_ref[pl.ds(12 * k, 12)]
            value = ext_ref[f, pair]
            moved = pltpu.roll(value, 16 * pair, 1) if pair else value
            place = (lane + (128 - 16 * pair)) % 64
            right = moved if right is None else jnp.where(place >= 52, moved, right)
            left = moved if left is None else jnp.where(place < 12, moved, left)
        right_ref[f] = right
        left_ref[f] = left


def coarse(gz_ref, ext_ref, low_ref, high_ref, old_ref, load_ref, weight_ref, s_ref, both_ref, out_ref,
           u1_ref, v1_ref, u2_ref, v2_ref, s2_ref, weight2_ref, state_ref, rest_ref, rows_ref, pair_ref, *work):
    work, fine_work = work[:5], work[5:]
    gz = gz_ref[0]
    lane = lane_index((ROWS, 128))
    clear_work(*work)
    clear_work(*fine_work)
    clear(u2_ref, v2_ref, weight2_ref)
    s2_ref[...] = jnp.zeros(s2_ref.shape, F32)
    for f in range(7):
        for z in (0, 9):
            v1_ref[f, z] = jnp.zeros((ROWS, 128), F32)
    for f in range(7):
        low, high = low_ref[f], high_ref[f]
        for pair in range(4):
            value = ext_ref[f, pair]
            for half in range(2):
                own = value if half == 0 else pltpu.roll(value, 64, 1)
                turn = (64 - 16 * pair - 64 * half) % 128
                below = pltpu.roll(low, turn, 1) if turn else low
                above = pltpu.roll(high, turn, 1) if turn else high
                whole = jnp.where(
                    lane < 64, own, jnp.where(lane < 64 + EDGE1, above, jnp.where(lane >= 128 - EDGE1, below, 0.0))
                )
                v1_ref[f, 1 + 2 * pair + half] = whole
    for c in range(3):
        for z in range(10):
            u1_ref[c, z] = v1_ref[4 + c, z] * v1_ref[c, z]

    s1_ref = v1_ref.at[3]
    sweep1 = smoother(u1_ref, v1_ref, v1_ref.at[pl.ds(4, 3)])
    stencil(u1_ref, s1_ref, sweep1, 1, 8, range(5), *work)

    def remain(z, t, forces):
        rows = pl.ds(8 * t, 8)
        for c in range(3):
            rest = v1_ref[c, z, rows, :] - forces[c]
            rest_ref[c, z, rows, :] = jnp.where(v1_ref[4 + c, z, rows, :] > 0, rest, 0.0)

    stencil(u1_ref, s1_ref, remain, 1, 8, range(5), *work)

    for z2 in range(4):
        z = 1 + 2 * z2
        for c in range(3):
            rest_ref[c, z] = rest_ref[c, z] + rest_ref[c, z + 1]
            rows_ref[pl.ds(24 * (4 * c + z2), 20)] = rest_ref[c, z, pl.ds(0, 20, 2), :] + rest_ref[c, z, pl.ds(1, 20, 2), :]
            rest_ref[c, 9] = jnp.where((v1_ref[4 + c, z] > 0) & (v1_ref[4 + c, z + 1] > 0), 1.0, 0.0)
            rows_ref[pl.ds(24 * (16 + 4 * c + z2), 20)] = jnp.minimum(
                rest_ref[c, 9, pl.ds(0, 20, 2), :], rest_ref[c, 9, pl.ds(1, 20, 2), :]
            )
        rest_ref[0, 9] = v1_ref[3, z] + v1_ref[3, z + 1]
        rows_ref[pl.ds(24 * (12 + z2), 20)] = rest_ref[0, 9, pl.ds(0, 20, 2), :] + rest_ref[0, 9, pl.ds(1, 20, 2), :]
    for k in range(28):
        rows_ref[pl.ds(24 * k + 20, 4)] = jnp.zeros((4, 128), F32)
    source = lax.broadcasted_iota(jnp.int32, (128, 128), 0)
    target = lax.broadcasted_iota(jnp.int32, (128, 128), 1)
    used = (target < 40) | (target >= 120)
    fold = (source // 2 + jnp.where(target < 64, 0, 64) == target) & used
    join = jnp.where(fold, 1.0, 0.0).astype(F32)
    level2 = jnp.dot(rows_ref[...], join, precision=lax.Precision.HIGHEST, preferred_element_type=F32)

    def part(k, z2):
        return level2[24 * (4 * k + z2): 24 * (4 * k + z2) + 24]

    for z2 in range(4):
        for c in range(3):
            v2_ref[c, 1 + z2] = part(c, z2)
            weight2_ref[c, 1 + z2] = jnp.where(part(4 + c, z2) > 1.5, 1.0, 0.0)
        s2_ref[1 + z2] = part(3, z2) * (4.0 / 2.0 / 8.0)
    weigh(s2_ref, weight2_ref, range(1, 5), range(3))
    for z in range(1, 5):
        for c in range(3):
            u2_ref[c, z] = weight2_ref[c, z] * v2_ref[c, z]

    sweep2 = smoother(u2_ref, v2_ref, weight2_ref)

    def again(k, carry):
        stencil(u2_ref, s2_ref, sweep2, 1, 4, range(3), *work)
        return carry

    lax.fori_loop(0, COARSE - 1, again, 0)

    part_of = jnp.where(
        (source == jnp.where(target < 96, target // 2, target // 2 + 64)), 1.0, 0.0
    ).astype(F32)
    for c in range(3):
        for z2 in range(4):
            rows_ref[pl.ds(24 * (4 * c + z2), 24)] = u2_ref[c, 1 + z2]
    spread = jnp.dot(rows_ref[pl.ds(0, 288)], part_of, precision=lax.Precision.HIGHEST, preferred_element_type=F32)
    for c in range(3):
        for z2 in range(4):
            k = 24 * (4 * c + z2)
            value = spread[k: k + 24][:20]
            rest_ref[c, 9, pl.ds(0, 20, 2), :] = value
            rest_ref[c, 9, pl.ds(1, 20, 2), :] = value
            for z in (1 + 2 * z2, 2 + 2 * z2):
                u1_ref[c, z] = u1_ref[c, z] + jnp.where(v1_ref[4 + c, z] > 0, rest_ref[c, 9], 0.0)

    for k in range(2):
        stencil(u1_ref, s1_ref, sweep1, 1 + 2 * gz + k * gz, 6 - k, range(1, 4), *work)

    start = 4 * gz
    lane8 = lane_index((8, 128))
    for c in range(3):
        for j in range(6):
            rows_ref[pl.ds(24 * (6 * c + j), 24)] = u1_ref[c, start + j, pl.ds(8, 24), :]
    target2 = lax.broadcasted_iota(jnp.int32, (128, 256), 1)
    source2 = lax.broadcasted_iota(jnp.int32, (128, 256), 0)
    copies = jnp.where(source2 == target2 // 2, 1.0, 0.0).astype(F32)
    fine = jnp.dot(rows_ref[pl.ds(0, 432)], copies, precision=lax.Precision.HIGHEST, preferred_element_type=F32)
    for c in range(3):
        for z in range(1, PLANES - 1):
            state_ref[c, z] = old_ref[c, z]
        for t in range(5):
            edges = both_ref[1 - gz, 43 + t]
            edges = pltpu.roll(edges, 128 - 8 * c, 1) if c else edges
            edges = jnp.where((lane8 < 4) | (lane8 >= 124), edges, 0.0)
            state_ref[c, 12 - 11 * gz, pl.ds(8 * t, 8), pl.ds(0, 128)] = both_ref[1 - gz, 28 + 5 * c + t]
            state_ref[c, 12 - 11 * gz, pl.ds(8 * t, 8), pl.ds(128, 128)] = edges
        for j in range(6):
            k = 24 * (6 * c + j)
            value = fine[k: k + 24][2:22]
            for k in range(2):
                here = pl.ds(128 * k, 128)
                pair_ref[k, pl.ds(0, 20, 2), :] = value[:, 128 * k: 128 * k + 128]
                pair_ref[k, pl.ds(1, 20, 2), :] = value[:, 128 * k: 128 * k + 128]
                for half in range(2):
                    z = 1 + 2 * j + half
                    state_ref[c, z, :, here] = state_ref[c, z, :, here] + jnp.where(
                        weight_ref[c, z, :, here] > 0, pair_ref[k], 0.0
                    )

    sweep = smoother(state_ref, load_ref, weight_ref)
    for k in range(2):
        stencil(state_ref, s_ref, sweep, 3 - gz + k * gz, 9 - k, range(5), *fine_work)
    for c in range(3):
        for z in range(8):
            out_ref[c, z] = state_ref[c, OWN + z, pl.ds(4, 32), pl.ds(0, 128)]


def up(value, axis):
    return lax.ppermute(value, axis, [(i, i + 1) for i in range(lax.axis_size(axis) - 1)])


def down(value, axis):
    return lax.ppermute(value, axis, [(i + 1, i) for i in range(lax.axis_size(axis) - 1)])


def swap(value):
    return lax.ppermute(value, "gz", [(0, 1), (1, 0)])


def scratch_of(rows, width, planes):
    parts = width // 128
    return [
        pltpu.VMEM((planes + 2, 6, parts, rows + 8, 128), F32),
        pltpu.VMEM((12, parts, rows, 128), F32),
        pltpu.VMEM((12, parts, rows, 128), F32),
        pltpu.VMEM((6, parts, rows + 8, 128), F32),
        pltpu.VMEM((planes + 1, 6, parts, rows, 128), F32),
    ]


def on_device(displacement, load, density_code, fixed_mask):
    gz = lax.axis_index("gz").astype(jnp.int32).reshape(1)
    block = (3, 8, 32, 128)
    zsend, base, right, left = call(
        prepare,
        [(24, 32, 128), (10, 8, 32, 128), (320, 128), (320, 128)],
        [gz, displacement, load, density_code, fixed_mask],
        [
            pltpu.VMEM(block, F32),
            pltpu.VMEM(block, F32),
            pltpu.VMEM(block[1:], jnp.int32),
            pltpu.VMEM(block, jnp.int32),
            pltpu.SemaphoreType.DMA((20,)),
        ],
        inputs="hbm",
    )
    zrecv = swap(zsend)
    low, high = up(right, "gx"), down(left, "gx")
    (zsend,) = call(boundary_rows, [(192, 128)], [gz, low, high])
    beside = lax.all_gather(zsend, "gz")
    ext, rising, falling = call(
        edge_lanes,
        [(10, PLANES, ROWS, 128), (4, ROWS, 128), (4, ROWS, 128)],
        [gz, base, zrecv, low, high, beside],
    )
    low, high = up(rising, "gy"), down(falling, "gy")
    wide = (3, PLANES, ROWS, LANES)
    tile, rest = (3, PLANES, ROWS, 128), (3, 8, ROWS, 128)
    main = call(fine_main, [tile, tile, rest], [gz, ext], scratch_of(ROWS, 128, 10))
    u, loads, weights, scales, send1 = call(
        fine_edges,
        [wide, wide, wide, (PLANES, ROWS, LANES), (48, 8, 128)],
        [gz, ext, low, high, *main],
        [
            pltpu.VMEM(tile, F32),
            pltpu.VMEM(tile, F32),
            pltpu.VMEM(tile, F32),
            pltpu.VMEM(tile[1:], F32),
            pltpu.VMEM(rest, F32),
            pltpu.VMEM(rest, F32),
            pltpu.VMEM((2, ROWS, 128), F32),
            pltpu.VMEM((256, 256), F32),
            pltpu.VMEM((104, ROWS, 128), F32),
        ]
        + scratch_of(ROWS, 128, 10),
    )
    both = lax.all_gather(send1, "gz")
    full, right, left = call(edge_rows1, [(7, 4, 16, 128), (336, 128), (336, 128)], [gz, both])
    low, high = up(right, "gx"), down(left, "gx")
    ext1, right, left = call(
        edge_lanes1, [(7, 4, ROWS, 128), (7, ROWS, 128), (7, ROWS, 128)], [gz, full, low, high]
    )
    low, high = up(right, "gy"), down(left, "gy")
    (out,) = call(
        coarse,
        [(3, 8, 32, 128)],
        [gz, ext1, low, high, u, loads, weights, scales, both],
        [
            pltpu.VMEM((3, 10, ROWS, 128), F32),
            pltpu.VMEM((7, 10, ROWS, 128), F32),
            pltpu.VMEM((3, 6, 24, 128), F32),
            pltpu.VMEM((3, 6, 24, 128), F32),
            pltpu.VMEM((6, 24, 128), F32),
            pltpu.VMEM((3, 6, 24, 128), F32),
            pltpu.VMEM(wide, F32),
            pltpu.VMEM((3, 10, ROWS, 128), F32),
            pltpu.VMEM((672, 128), F32),
            pltpu.VMEM((2, ROWS, 128), F32),
        ]
        + scratch_of(ROWS, 128, 8)
        + scratch_of(ROWS, LANES, 9),
        output="plain",
    )
    return out


def solution(mesh):
    return jax.shard_map(
        on_device,
        mesh=mesh,
        in_specs=(
            P(None, "gz", "gx", "gy"),
            P(None, "gz", "gx", "gy"),
            P("gz", "gx", "gy"),
            P(None, "gz", "gx", "gy"),
        ),
        out_specs=P(None, "gz", "gx", "gy"),
        check_vma=False,
    )
```
